128 devices in a mesh: slab: 32 (over y, x, core), site: 4 (over z).
Axes of the slice: x: 4, y: 4, z: 4, core: 2. Of those that a mesh axis runs over, the one named last changes fastest.
Arguments:
- potential: float32 [3, 256, 256, 256], P(None, 'slab', 'site'), may hold values from -12 to 12
- t_now: float32 [3, 256, 256, 256], P(None, 'slab', 'site'), may hold values from -3 to 3
- hist_t: float32 [4, 3, 256, 256, 256], P(None, None, 'slab', 'site'), may hold values from -3 to 3
- hist_r: float32 [4, 3, 256, 256, 256], P(None, None, 'slab', 'site'), may hold values from -15 to 15
- chi_self: float32 [3, 256, 256, 256], P(None, ('slab', 'site')), may hold values from 0.3 to 3, as said below
- chi_cross: float32 [3, 256, 256, 256], P(None, ('slab', 'site')), may hold values from -1.8 to 1.8, as said below
Outputs:
- t_next: float32 [3, 256, 256, 256], P(None, 'slab', 'site')
- residual_last: float32 [3, 256, 256, 256], P(None, 'slab', 'site')
The draws below stay inside these ranges and needn't reach their ends.
Inputs may be any that keep to these rules, and one draw needn't show every extreme that they name: `chi_self`: even in the wave vector: the entry at (kx, ky, kz) equals that at (-kx, -ky, -kz), indices taken modulo the grid. `chi_cross`: even in the wave vector: the entry at (kx, ky, kz) equals that at (-kx, -ky, -kz), indices taken modulo the grid.
All inputs are finite; a program needn't handle non-finite values.
Results may differ from the reference program's by a relative error of at most 0.0003.
Values sent between devices are 32-bit elements; how exact they have to be, the bound alone decides.
A program may use at most 192 MiB of HBM per device.

```python
import math
import jax
import jax.numpy as jnp
import numpy as np
from jax import lax

NX = 256
NY = 256
NZ = 256
SITES = 3
ITERS = 1
HIST = 4
N_SLAB = 32
N_SITE = 4


def wave_order_drawn(depth, devices):
    half_block = depth // (2 * devices)
    rows = np.arange(depth)
    block = rows // (2 * half_block)
    within = rows % (2 * half_block)
    lower = within < half_block
    base = block * half_block + np.where(lower, within, within - half_block)
    partner = np.where(base == 0, depth // 2, depth - base)
    return np.where(lower, base, partner)


def make_even(values):
    mirrored = jnp.roll(jnp.flip(values, (1, 2, 3)), 1, (1, 2, 3))
    even = 0.5 * (values + mirrored)
    order = jnp.asarray(wave_order_drawn(NZ, N_SLAB * N_SITE), jnp.int32)
    return jnp.take(even, order, axis=1)


def position_ramp():
    leading = jnp.arange(NX, dtype=jnp.float32) / (NX - 1)
    trailing = jnp.arange(NY, dtype=jnp.float32) / (NY - 1)
    return 0.5 * (leading[:, None, None] + trailing[None, :, None])


def draw_potential(key, part):
    extent = (SITES, NX, NY, NZ)
    amplitude = jnp.exp(math.log(3.0) * position_ramp())
    values = jnp.clip(jax.random.normal(key, extent, jnp.float32), -4.0, 4.0)
    return values * amplitude[None]


def draw_hist_r(key, part):
    extent = (HIST, SITES, NX, NY, NZ)
    position = position_ramp()[None, None]
    member = jnp.arange(HIST)
    rising = (member % 2 == 0)[:, None, None, None, None]
    amplitude = jnp.exp(math.log(3.0) * jnp.where(rising, position, 1.0 - position))
    own_key = jax.random.fold_in(key, 11)
    values = jnp.clip(jax.random.normal(own_key, extent, jnp.float32), -5.0, 5.0)
    return values * amplitude


def draw_chi_self(key, part):
    extent = (SITES, NZ, NY, NX)
    own_key = jax.random.fold_in(key, 31)
    exponent = jax.random.uniform(own_key, extent, jnp.float32, math.log(0.3), math.log(3.0))
    values = jnp.exp(exponent)
    return make_even(values)


def draw_chi_cross(key, part):
    extent = (SITES, NZ, NY, NX)
    own_key = jax.random.fold_in(key, 47)
    values = 0.3 * jnp.clip(jax.random.normal(own_key, extent, jnp.float32), -6.0, 6.0)
    return make_even(values)


def levels(rng, shape, cuts, low, largest):
    level = 1.0
    for dim, shards_of in cuts:
        steps = jax.random.uniform(jax.random.fold_in(jax.random.fold_in(rng, 6), dim), (shards_of,), jnp.float32, low / len(cuts), largest / len(cuts))
        level = level * jnp.repeat(jnp.exp(steps), shape[dim] // shards_of).reshape((-1,) + (1,) * (len(shape) - 1 - dim))
    return level


def bell_draw(rng, shape, scale, bound, shards=(), kind=jnp.bfloat16):
    loudness = levels(rng, shape, shards, -0.22, 0.18) if shards else 1.0
    entries = jax.random.normal(rng, shape, jnp.float32) * scale * loudness
    return jnp.minimum(jnp.maximum(entries, -bound), bound).astype(kind)


def setup_inputs(seed: int = 0) -> dict:
    splits = jax.random.split(jax.random.key(seed), 7)
    potential = draw_potential(jax.random.fold_in(splits[6], 71), 0)
    t_now = bell_draw(splits[1], (SITES, NX, NY, NZ), 0.5, 3.0, ((1, 32), (2, 4)), jnp.float32)
    hist_t = bell_draw(splits[2], (HIST, SITES, NX, NY, NZ), 0.5, 3.0, ((2, 32), (3, 4)), jnp.float32)
    hist_r = draw_hist_r(jax.random.fold_in(splits[6], 71), 0)
    chi_self = draw_chi_self(jax.random.fold_in(splits[6], 71), 0)
    chi_cross = draw_chi_cross(jax.random.fold_in(splits[6], 71), 0)
    return dict(potential=potential, t_now=t_now, hist_t=hist_t, hist_r=hist_r, chi_self=chi_self, chi_cross=chi_cross)


MIXING = 0.5

def wave_order(depth, devices):
    half_block = depth // (2 * devices)
    rows = np.arange(depth)
    block = rows // (2 * half_block)
    within = rows % (2 * half_block)
    lower = within < half_block
    base = block * half_block + np.where(lower, within, within - half_block)
    partner = np.where(base == 0, depth // 2, depth - base)
    return np.where(lower, base, partner)

def closure(indirect, potential):
    field_value = indirect - potential
    totals = jnp.where(field_value > 0, field_value, jnp.expm1(jnp.minimum(field_value, 0.0)))
    return totals - indirect

def combine_sites(values, self_part, cross_part):
    site_zero, site_one, site_two = (values[0], values[1], values[2])
    out_zero = self_part[0] * site_zero + cross_part[0] * site_one + cross_part[1] * site_two
    out_one = cross_part[0] * site_zero + self_part[1] * site_one + cross_part[2] * site_two
    out_two = cross_part[1] * site_zero + cross_part[2] * site_one + self_part[2] * site_two
    return jnp.stack([out_zero, out_one, out_two])

def residual_of(indirect, potential, self_turned, cross_turned):
    direct_corr = closure(indirect, potential)
    spectrum = jnp.fft.fftn(direct_corr, axes=(1, 2, 3))
    mixed = combine_sites(spectrum, self_turned, cross_turned)
    total_new = jnp.real(jnp.fft.ifftn(mixed, axes=(1, 2, 3))).astype(indirect.dtype)
    return total_new - direct_corr - indirect

def solve_weights(gram):
    count = gram.shape[0]
    factor = [[None] * count for member in range(count)]
    for column in range(count):
        diagonal_sum = gram[column, column]
        for inner in range(column):
            diagonal_sum = diagonal_sum - factor[column][inner] * factor[column][inner]
        factor[column][column] = jnp.sqrt(diagonal_sum)
        for row in range(column + 1, count):
            entry = gram[row, column]
            for inner in range(column):
                entry = entry - factor[row][inner] * factor[column][inner]
            factor[row][column] = entry / factor[column][column]
    middle = []
    for row in range(count):
        entry = jnp.ones((), gram.dtype)
        for inner in range(row):
            entry = entry - factor[row][inner] * middle[inner]
        middle.append(entry / factor[row][row])
    weights = [None] * count
    for row in range(count - 1, -1, -1):
        entry = middle[row]
        for inner in range(row + 1, count):
            entry = entry - factor[inner][row] * weights[inner]
        weights[row] = entry / factor[row][row]
    stacked = jnp.stack(weights)
    return stacked / jnp.sum(stacked)

def extrapolate(iterates, residuals):
    stacked = jnp.stack(residuals).reshape(len(residuals), -1)
    gram = jnp.dot(stacked, stacked.T, precision=lax.Precision.HIGHEST, preferred_element_type=jnp.float32)
    weights = solve_weights(gram)
    result = weights[0] * (iterates[0] + MIXING * residuals[0])
    for member in range(1, len(iterates)):
        result = result + weights[member] * (iterates[member] + MIXING * residuals[member])
    return result

def reference(potential, t_now, hist_t, hist_r, chi_self, chi_cross):
    order = wave_order(NZ, N_SLAB * N_SITE)
    inverse_rows = jnp.asarray(np.argsort(order), jnp.int32)
    self_turned = jnp.transpose(jnp.take(chi_self, inverse_rows, axis=1), (0, 3, 2, 1))
    cross_turned = jnp.transpose(jnp.take(chi_cross, inverse_rows, axis=1), (0, 3, 2, 1))
    iterates = [hist_t[member] for member in range(HIST)]
    residuals = [hist_r[member] for member in range(HIST)]
    indirect = t_now
    latest = t_now
    for iteration in range(ITERS):
        latest = residual_of(indirect, potential, self_turned, cross_turned)
        iterates = iterates + [indirect]
        residuals = residuals + [latest]
        indirect = extrapolate(iterates, residuals)
        iterates = iterates[1:]
        residuals = residuals[1:]
    return (indirect, latest)
```

```python
import functools
import math

import jax
import jax.numpy as jnp
import numpy as np
from jax import lax
from jax.experimental import pallas as pl
from jax.experimental.pallas import tpu as pltpu
from jax.sharding import PartitionSpec as P

N = 256
HALF = N // 2
SITES = 3
HIST = 4
MIXING = 0.5
MESH = pl.DeviceIdType.MESH
F32 = jnp.float32
BF16 = jnp.bfloat16

ROWS = 512
PEERS = 127

NT = (((1,), (1,)), ((), ()))
NN = (((1,), (0,)), ((), ()))


def split_table(table):
    high = table.astype(np.float32).astype(jnp.bfloat16)
    low = (table - high.astype(np.float64)).astype(np.float32).astype(jnp.bfloat16)
    return np.stack([high, low])


def tables():
    index = np.arange(N)
    angles = (index[:, None] * index[None, :] % N) * (2.0 * math.pi / N)
    cosine, sine = np.cos(angles), np.sin(angles)
    imag_rows = -sine[:HALF].copy()
    imag_rows[0] = 1.0 - 2.0 * (index % 2)
    along_z = np.concatenate([cosine[:HALF], imag_rows], 0)
    along_x = np.concatenate([cosine, sine], 0)
    blocks = np.stack([cosine.reshape(N, 4, 64), sine.reshape(N, 4, 64)], 2).reshape(N, 512)
    turned = np.stack([-sine.reshape(N, 4, 64), cosine.reshape(N, 4, 64)], 2).reshape(N, 512)
    along_y = np.concatenate([blocks, turned], 0)
    return split_table(along_z), split_table(along_x), split_table(along_y)


def halves(value):
    high = value.astype(BF16)
    low = (value - high.astype(F32)).astype(BF16)
    return high, low


def solve_weights(gram):
    count = HIST + 1
    factor = [[None] * count for member in range(count)]
    for column in range(count):
        diagonal_sum = gram[column][column]
        for inner in range(column):
            diagonal_sum = diagonal_sum - factor[column][inner] * factor[column][inner]
        factor[column][column] = jnp.sqrt(diagonal_sum)
        for row in range(column + 1, count):
            entry = gram[row][column]
            for inner in range(column):
                entry = entry - factor[row][inner] * factor[column][inner]
            factor[row][column] = entry / factor[column][column]
    middle = []
    for row in range(count):
        entry = jnp.ones_like(gram[0][0])
        for inner in range(row):
            entry = entry - factor[row][inner] * middle[inner]
        middle.append(entry / factor[row][row])
    weights = [None] * count
    for row in range(count - 1, -1, -1):
        entry = middle[row]
        for inner in range(row + 1, count):
            entry = entry - factor[inner][row] * weights[inner]
        weights[row] = entry / factor[row][row]
    total = weights[0]
    for row in range(1, count):
        total = total + weights[row]
    return [weight / total for weight in weights]


PAIRS = [(i, j) for i in range(HIST) for j in range(i, HIST)]


def kernel(
    pot_hbm, t_hbm, hist_t_hbm, hist_r_hbm, self_hbm, cross_hbm, wz_hbm, cs_hbm, h_hbm,
    next_hbm, last_hbm,
    tv, hv, ut, hr, low_chi, top_chi,
    wz_wide, wz_tall, cs_wide, h_wide, h_tall,
    sent, got, spec, spec_top, back, home,
    d_b, z_f, r_b, zz_f, u_b, m_b, t_b, e_b, y_f,
    g_row, g_one, g_mid, g_two, res,
    in_sem, out_sem, fsend, frecv, bsend, brecv, gsend, grecv,
):
    slab = lax.axis_index("slab")
    site = lax.axis_index("site")
    plane = slab // 2
    py, px, core = plane // 4, plane % 4, slab % 2
    me = slab * 4 + site
    leading = me == 0

    counter = [0]
    copies = {}

    def load(name, src, dst):
        copy = pltpu.make_async_copy(src, dst, in_sem.at[counter[0]])
        counter[0] += 1
        copies[name] = copy
        copy.start()

    for q in range(SITES):
        load(("t", q), t_hbm.at[q], tv.at[q])
        load(("p", q), pot_hbm.at[q], hv.at[q])
        if q == 0:
            load("wz0", wz_hbm.at[0], wz_wide.at[:, pl.ds(0, 256)])
            load("wz1", wz_hbm.at[1], wz_wide.at[:, pl.ds(256, 256)])
            load("wz2", wz_hbm.at[0], wz_wide.at[:, pl.ds(512, 256)])
    load("r", hist_r_hbm, hr)
    load("u", hist_t_hbm, ut)
    for part in range(3):
        load(("cs", part), cs_hbm.at[part % 2], cs_wide.at[:, pl.ds(256 * part, 256)])
        load(("hw", part), h_hbm.at[part % 2], h_wide.at[:, pl.ds(512 * part, 512)])
    for a in range(SITES):
        load(("sl", a), self_hbm.at[a, 0], low_chi.at[a])
        load(("cl", a), cross_hbm.at[a, 0], low_chi.at[3 + a])
        load(("st", a), self_hbm.at[a, 1], top_chi.at[a])
        load(("ct", a), cross_hbm.at[a, 1], top_chi.at[3 + a])
    for part in range(3):
        load(("ht", part), h_hbm.at[part % 2], h_tall.at[pl.ds(512 * part, 512)])
        load(("wt", part), wz_hbm.at[part % 2], wz_tall.at[pl.ds(256 * part, 256)])

    cores = [core, (core + 1) % 2]
    zs = [(site + step) % 4 for step in range(4)]

    def chip(group):
        return ((py + group // 4) % 4) * 4 + (px + group % 4) % 4

    def over_peers(action):
        base = chip(0) * 2
        for near in range(1, 8):
            action(base + cores[near // 4], zs[near % 4])

        def step(group, carry):
            base = chip(group) * 2
            for near in range(8):
                action(base + cores[near // 4], zs[near % 4])
            return carry

        lax.fori_loop(1, 16, step, 0)

    barrier = pltpu.get_barrier_semaphore()
    over_peers(
        lambda sl, st: pl.semaphore_signal(
            barrier, inc=1, device_id=(sl, st), device_id_type=MESH
        )
    )

    lane = lax.broadcasted_iota(jnp.int32, (1, 128), 1)
    real_half = lane < 64

    def swap(value):
        return pltpu.roll(value, 64, 1)

    def forward_site(q):
        def chunk(c, carry):
            rows = pl.ds(pl.multiple_of(c * 64, 64), 64)
            indirect = tv[q, rows, :]
            field = indirect - hv[q, rows, :]
            total = jnp.where(field > 0, field, jnp.exp(jnp.minimum(field, 0.0)) - 1.0)
            hv[q, rows, :] = total
            high, low = halves(total - indirect)
            d_b[rows, 0:256] = high
            d_b[rows, 256:512] = high
            d_b[rows, 512:768] = low
            return carry

        lax.fori_loop(0, ROWS // 64, chunk, 0)
        z_f[...] = lax.dot_general(wz_wide[...], d_b[...], NT, preferred_element_type=F32)
        for pair in range(4):
            columns = pl.ds(128 * pair, 128)
            real, imag = z_f[0:128, columns], z_f[128:256, columns]
            first = jnp.where(real_half, real, swap(imag))
            second = jnp.where(real_half, swap(real), imag)
            sent[q, pl.ds(2 * pair, 128, stride=8), :] = first
            sent[q, pl.ds(2 * pair + 1, 128, stride=8), :] = second

    def send_forward(q):
        def action(sl, st):
            wave = pl.multiple_of((sl * 4 + st) * 8, 8)
            pltpu.make_async_remote_copy(
                src_ref=sent.at[q, pl.ds(wave, 8)],
                dst_ref=got.at[q, site, pl.ds(pl.multiple_of(slab * 8, 8), 8)],
                send_sem=fsend.at[q],
                recv_sem=frecv.at[q],
                device_id=(sl, st),
                device_id_type=MESH,
            ).start()

        over_peers(action)
        got[q, site, pl.ds(pl.multiple_of(slab * 8, 8), 8), :] = sent[
            q, pl.ds(pl.multiple_of(me * 8, 8), 8), :
        ]

    for q in range(SITES):
        copies[("t", q)].wait()
        copies[("p", q)].wait()
        if q == 0:
            for part in range(3):
                copies[f"wz{part}"].wait()
        forward_site(q)
        if q == 0:
            pl.semaphore_wait(barrier, PEERS)
        send_forward(q)

    copies["r"].wait()
    copies["u"].wait()

    def history(c, sums):
        rows = pl.ds(pl.multiple_of(c * 8, 8), 8)
        rs = [hr[i, rows, :] for i in range(HIST)]
        for i in range(HIST):
            ut[i, rows, :] = ut[i, rows, :] + MIXING * rs[i]
        return tuple(s + rs[i] * rs[j] for s, (i, j) in zip(sums, PAIRS))

    zero = jnp.zeros((8, 256), F32)
    past = lax.fori_loop(0, SITES * ROWS // 8, history, (zero,) * len(PAIRS))
    for part in range(3):
        copies[("cs", part)].wait()
        copies[("hw", part)].wait()
        copies[("ht", part)].wait()
        copies[("wt", part)].wait()
    for a in range(SITES):
        for kind in ("sl", "cl", "st", "ct"):
            copies[(kind, a)].wait()

    def arrived(sem):
        block = sent.at[0, pl.ds(0, PEERS * 8)]
        pltpu.make_async_copy(block, block, sem).wait()

    def along_y(pick, target, q):
        for s in range(4):
            columns = pl.ds(128 * s, 128)
            one, two = zz_f[0:256, columns], zz_f[256:512, columns]
            high, low = halves(pick(one, two))
            u_b[:, pl.ds(128 * s, 128)] = high
            u_b[:, pl.ds(512 + 128 * s, 128)] = high
            u_b[:, pl.ds(1024 + 128 * s, 128)] = low
        target[q] = lax.dot_general(h_wide[...], u_b[...], NT, preferred_element_type=F32)

    def pick_whole(one, two):
        other = swap(two)
        return one + jnp.where(real_half, other, -other)

    def pick_low(one, two):
        return jnp.where(real_half, one, -swap(two))

    def pick_top(one, two):
        return jnp.where(real_half, swap(one), -two)

    def plane_site(q, carry):
        arrived(frecv.at[q])
        for s in range(4):
            columns = pl.ds(128 * s, 128)
            high, low = halves(got[q, s])
            r_b[0:256, columns] = high
            r_b[256:512, columns] = high
            r_b[512:768, columns] = low
        zz_f[...] = lax.dot_general(cs_wide[...], r_b[...], NN, preferred_element_type=F32)

        @pl.when(leading)
        def _():
            along_y(pick_low, spec, q)
            along_y(pick_top, spec_top, q)

        @pl.when(jnp.logical_not(leading))
        def _():
            along_y(pick_whole, spec, q)

        return carry

    lax.fori_loop(0, SITES, plane_site, 0)

    def combine(chi, field, a, rows, upper):
        total = None
        for g in range(SITES):
            entry = chi[jnp.where(a == g, a, a + g + 2), rows, :]
            term = entry * field[g, upper, :]
            total = term if total is None else total + term
        return total

    def store_mixed(rows, value):
        high, low = halves(value)
        m_b[rows, 0:256] = high
        m_b[rows, 256:512] = high
        m_b[rows, 512:768] = low

    def back_site(a, carry):
        def mix(c, carry):
            rows = pl.ds(pl.multiple_of(c * 32, 32), 32)
            lower = pl.ds(pl.multiple_of(256 + c * 32, 32), 32)
            real = combine(low_chi, spec, a, rows, rows)
            imag = combine(low_chi, spec, a, rows, lower)

            @pl.when(leading)
            def _():
                top_real = combine(top_chi, spec_top, a, rows, rows)
                top_imag = combine(top_chi, spec_top, a, rows, lower)
                store_mixed(rows, (real - top_imag) * (1.0 / N**3))
                store_mixed(lower, (imag + top_real) * (1.0 / N**3))

            @pl.when(jnp.logical_not(leading))
            def _():
                store_mixed(rows, real * (2.0 / N**3))
                store_mixed(lower, imag * (2.0 / N**3))

            return carry

        lax.fori_loop(0, 8, mix, 0)
        zz_f[...] = lax.dot_general(cs_wide[...], m_b[...], NT, preferred_element_type=F32)
        for block in range(4):
            rows, lower = pl.ds(64 * block, 64), pl.ds(256 + 64 * block, 64)
            real = zz_f[rows, 0:256] - zz_f[lower, 256:512]
            imag = zz_f[rows, 256:512] + zz_f[lower, 0:256]
            for place, value in ((0, real), (256, imag)):
                high, low = halves(value)
                t_b[rows, pl.ds(place, 256)] = high
                t_b[rows, pl.ds(512 + place, 256)] = high
                t_b[rows, pl.ds(1024 + place, 256)] = low
        planes = lax.dot_general(t_b[...], h_tall[...], NN, preferred_element_type=F32)
        for s in range(4):
            back[a, s] = planes[:, 128 * s : 128 * s + 128]

        def action(sl, st):
            pltpu.make_async_remote_copy(
                src_ref=back.at[a, st, pl.ds(pl.multiple_of(sl * 8, 8), 8)],
                dst_ref=home.at[a, pl.ds(pl.multiple_of(me * 8, 8), 8)],
                send_sem=bsend.at[a],
                recv_sem=brecv.at[a],
                device_id=(sl, st),
                device_id_type=MESH,
            ).start()

        over_peers(action)
        home[a, pl.ds(pl.multiple_of(me * 8, 8), 8), :] = back[
            a, site, pl.ds(pl.multiple_of(slab * 8, 8), 8), :
        ]
        return carry

    lax.fori_loop(0, SITES, back_site, 0)

    def home_site(a, sums):
        arrived(brecv.at[a])
        for x in range(8):
            lines = jnp.transpose(home[a, pl.ds(x, 128, stride=8), :])
            high, low = halves(jnp.concatenate([lines[0:64], lines[64:128]], 1))
            rows = pl.ds(64 * x, 64)
            e_b[rows, 0:256] = high
            e_b[rows, 256:512] = high
            e_b[rows, 512:768] = low
        y_f[...] = lax.dot_general(e_b[...], wz_tall[...], NN, preferred_element_type=F32)

        def chunk(c, sums):
            rows = pl.ds(pl.multiple_of(c * 8, 8), 8)
            latest = y_f[rows, :] - hv[a, rows, :]
            hv[a, rows, :] = latest
            tv[a, rows, :] = tv[a, rows, :] + MIXING * latest
            offset = pl.ds(pl.multiple_of(a * ROWS + c * 8, 8), 8)
            new = [s + hr[i, offset, :] * latest for i, s in enumerate(sums[:HIST])]
            return tuple(new) + (sums[HIST] + latest * latest,)

        sums = lax.fori_loop(0, ROWS // 8, chunk, sums)
        pltpu.make_async_copy(hv.at[a], last_hbm.at[a], out_sem.at[a]).start()
        return sums

    newest = lax.fori_loop(0, SITES, home_site, (zero,) * (HIST + 1))

    entries = {pair: s for pair, s in zip(PAIRS, past)}
    for i in range(HIST + 1):
        entries[(i, HIST)] = newest[i]
    order = sorted(entries)
    row = jnp.zeros((1, 128), F32)
    for place, pair in enumerate(order):
        folded = entries[pair][:, 0:128] + entries[pair][:, 128:256]
        value = jnp.sum(jnp.sum(folded, axis=0, keepdims=True), axis=1, keepdims=True)
        row = jnp.where(lane == place, value, row)
    g_row[0:1, :] = row

    def send_row(src, dst, slot, stage, sl, st):
        pltpu.make_async_remote_copy(
            src_ref=src.at[pl.ds(0, 1)],
            dst_ref=dst.at[pl.ds(slot, 1)],
            send_sem=gsend.at[stage],
            recv_sem=grecv.at[stage],
            device_id=(sl, st),
            device_id_type=MESH,
        ).start()

    for near in range(1, 2):
        send_row(g_row, g_one, slab, 0, chip(0) * 2 + cores[near], site)

    def spread(group, carry):
        for near in range(2):
            send_row(g_row, g_one, slab, 0, chip(group) * 2 + cores[near], site)
        return carry

    lax.fori_loop(1, 16, spread, 0)
    g_one[pl.ds(slab, 1), :] = row

    def wait_rows(count, sem):
        block = g_one.at[pl.ds(0, count)]
        pltpu.make_async_copy(block, block, sem).wait()

    wait_rows(31, grecv.at[0])
    partial = jnp.sum(g_one[...], axis=0, keepdims=True)
    g_mid[0:1, :] = partial
    for near in range(1, 4):
        send_row(g_mid, g_two, site, 1, slab, zs[near])
    g_two[pl.ds(site, 1), :] = partial
    wait_rows(3, grecv.at[1])
    whole = (g_two[0:1, :] + g_two[1:2, :]) + (g_two[2:3, :] + g_two[3:4, :])

    gram = [[None] * (HIST + 1) for i in range(HIST + 1)]
    for place, (i, j) in enumerate(order):
        value = jnp.sum(jnp.where(lane == place, whole, 0.0), axis=1, keepdims=True)
        gram[i][j] = gram[j][i] = jnp.broadcast_to(value, (1, 128))
    weights = [
        jnp.broadcast_to(jnp.concatenate([weight, weight], 1), (8, 256))
        for weight in solve_weights(gram)
    ]

    for a in range(SITES):

        def finish(c, carry):
            rows = pl.ds(pl.multiple_of(c * 8, 8), 8)
            offset = pl.ds(pl.multiple_of(a * ROWS + c * 8, 8), 8)
            value = weights[0] * ut[0, offset, :]
            for i in range(1, HIST):
                value = value + weights[i] * ut[i, offset, :]
            res[a, rows, :] = value + weights[HIST] * tv[a, rows, :]
            return carry

        lax.fori_loop(0, ROWS // 8, finish, 0, unroll=4)
        pltpu.make_async_copy(res.at[a], next_hbm.at[a], out_sem.at[SITES + a]).start()

    for q in range(SITES):
        arrived(fsend.at[q])
        arrived(bsend.at[q])
    wait_rows(31, gsend.at[0])
    wait_rows(3, gsend.at[1])
    for a in range(SITES):
        pltpu.make_async_copy(hv.at[a], last_hbm.at[a], out_sem.at[a]).wait()
        pltpu.make_async_copy(res.at[a], next_hbm.at[a], out_sem.at[SITES + a]).wait()


def step(potential, t_now, hist_t, hist_r, chi_self, chi_cross):
    flat = (SITES, ROWS, N)
    wz, cs, hh = tables()
    vm = pltpu.VMEM
    field = jax.ShapeDtypeStruct(flat, F32)
    scratch = [
        vm(flat, F32), vm(flat, F32),
        vm((HIST, SITES * ROWS, N), F32), vm((HIST, SITES * ROWS, N), F32),
        vm((6, N, N), F32), vm((6, N, N), F32),
        vm((256, 768), BF16), vm((768, 256), BF16), vm((512, 768), BF16),
        vm((512, 1536), BF16), vm((1536, 512), BF16),
        vm((SITES, 1024, 128), F32), vm((SITES, 4, 256, 128), F32),
        vm((SITES, 512, 256), F32), vm((SITES, 512, 256), F32),
        vm((SITES, 4, 256, 128), F32), vm((SITES, 1024, 128), F32),
        vm((512, 768), BF16), vm((256, 512), F32), vm((768, 512), BF16),
        vm((512, 512), F32), vm((256, 1536), BF16), vm((512, 768), BF16),
        vm((256, 1536), BF16), vm((512, 768), BF16), vm((512, 256), F32),
        vm((8, 128), F32), vm((32, 128), F32), vm((8, 128), F32), vm((8, 128), F32),
        vm(flat, F32),
        pltpu.SemaphoreType.DMA((40,)), pltpu.SemaphoreType.DMA((6,)),
        pltpu.SemaphoreType.DMA((3,)), pltpu.SemaphoreType.DMA((3,)),
        pltpu.SemaphoreType.DMA((3,)), pltpu.SemaphoreType.DMA((3,)),
        pltpu.SemaphoreType.DMA((2,)), pltpu.SemaphoreType.DMA((2,)),
    ]
    anywhere = pl.BlockSpec(memory_space=pl.ANY)
    t_next, residual = pl.pallas_call(
        kernel,
        out_shape=(field, field),
        in_specs=[anywhere] * 9,
        out_specs=(anywhere, anywhere),
        scratch_shapes=scratch,
        compiler_params=pltpu.CompilerParams(
            collective_id=0, has_side_effects=True, vmem_limit_bytes=56 * 1024 * 1024
        ),
    )(
        potential.reshape(flat),
        t_now.reshape(flat),
        hist_t.reshape(HIST, SITES * ROWS, N),
        hist_r.reshape(HIST, SITES * ROWS, N),
        chi_self,
        chi_cross,
        jnp.asarray(wz),
        jnp.asarray(cs),
        jnp.asarray(hh),
    )
    return t_next.reshape(t_now.shape), residual.reshape(t_now.shape)


def solution(mesh):
    field = P(None, "slab", "site", None)
    past = P(None, None, "slab", "site", None)
    chi = P(None, ("slab", "site"), None, None)
    return jax.shard_map(
        step,
        mesh=mesh,
        in_specs=(field, field, past, past, chi, chi),
        out_specs=(field, field),
        check_vma=False,
    )
```

```python
import functools
import math

import jax
import jax.numpy as jnp
import numpy as np
from jax import lax
from jax.experimental import pallas as pl
from jax.experimental.pallas import tpu as pltpu
from jax.sharding import PartitionSpec as P

N = 256
HALF = N // 2
SITES = 3
HIST = 4
MIXING = 0.5
MESH = pl.DeviceIdType.MESH
F32 = jnp.float32
BF16 = jnp.bfloat16

ROWS = 512
PEERS = 127

NT = (((1,), (1,)), ((), ()))
NN = (((1,), (0,)), ((), ()))


def split_table(table):
    high = table.astype(np.float32).astype(jnp.bfloat16)
    low = (table - high.astype(np.float64)).astype(np.float32).astype(jnp.bfloat16)
    return np.stack([high, low])


def tables():
    index = np.arange(N)
    angles = (index[:, None] * index[None, :] % N) * (2.0 * math.pi / N)
    cosine, sine = np.cos(angles), np.sin(angles)
    imag_rows = -sine[:HALF].copy()
    imag_rows[0] = 1.0 - 2.0 * (index % 2)
    along_z = np.concatenate([cosine[:HALF], imag_rows], 0)
    along_x = np.concatenate([cosine, sine], 0)
    blocks = np.stack([cosine.reshape(N, 4, 64), sine.reshape(N, 4, 64)], 2).reshape(N, 512)
    turned = np.stack([-sine.reshape(N, 4, 64), cosine.reshape(N, 4, 64)], 2).reshape(N, 512)
    along_y = np.concatenate([blocks, turned], 0)
    waves = np.arange(HALF).reshape(16, 2, 4)
    cuts = [split_table(along_z[np.concatenate([w, w + HALF])]) for w in (waves[:, c].ravel() for c in (0, 1))]
    from_z = np.stack([np.concatenate([cut[0], cut[1], cut[0]], 0) for cut in cuts])
    return split_table(along_z), split_table(along_x), split_table(along_y), from_z


def halves(value):
    high = value.astype(BF16)
    low = (value - high.astype(F32)).astype(BF16)
    return high, low


def solve_weights(gram):
    count = HIST + 1
    factor = [[None] * count for member in range(count)]
    for column in range(count):
        diagonal_sum = gram[column][column]
        for inner in range(column):
            diagonal_sum = diagonal_sum - factor[column][inner] * factor[column][inner]
        factor[column][column] = jnp.sqrt(diagonal_sum)
        for row in range(column + 1, count):
            entry = gram[row][column]
            for inner in range(column):
                entry = entry - factor[row][inner] * factor[column][inner]
            factor[row][column] = entry / factor[column][column]
    middle = []
    for row in range(count):
        entry = jnp.ones_like(gram[0][0])
        for inner in range(row):
            entry = entry - factor[row][inner] * middle[inner]
        middle.append(entry / factor[row][row])
    weights = [None] * count
    for row in range(count - 1, -1, -1):
        entry = middle[row]
        for inner in range(row + 1, count):
            entry = entry - factor[inner][row] * weights[inner]
        weights[row] = entry / factor[row][row]
    total = weights[0]
    for row in range(1, count):
        total = total + weights[row]
    return [weight / total for weight in weights]


PAIRS = [(i, j) for i in range(HIST) for j in range(i, HIST)]


def kernel(
    pot_hbm, t_hbm, hist_t_hbm, hist_r_hbm, self_hbm, cross_hbm, wz_hbm, cs_hbm, h_hbm, wb_hbm,
    next_ref, last_ref,
    tv, hv, ut, hr, low_chi, top_chi,
    wz_wide, w_back, cs_wide, h_wide, h_tall,
    sent, got, spec, spec_top, back, home,
    d_b, z_f, r_b, zz_f, u_b, m_b, t_b, e_b, y_f,
    g_row, g_all,
    in_sem, fsend, frecv, bsend, brecv, gsend, grecv,
):
    slab = lax.axis_index("slab")
    site = lax.axis_index("site")
    plane = slab // 2
    py, px, core = plane // 4, plane % 4, slab % 2
    me = slab * 4 + site
    leading = me == 0

    counter = [0]
    copies = {}

    def load(name, src, dst):
        copy = pltpu.make_async_copy(src, dst, in_sem.at[counter[0]])
        counter[0] += 1
        copies[name] = copy
        copy.start()

    for q in range(SITES):
        load(("t", q), t_hbm.at[q], tv.at[q])
        load(("p", q), pot_hbm.at[q], hv.at[q])
        if q == 0:
            load("wz0", wz_hbm.at[0], wz_wide.at[:, pl.ds(0, 256)])
            load("wz1", wz_hbm.at[1], wz_wide.at[:, pl.ds(256, 256)])
            load("wz2", wz_hbm.at[0], wz_wide.at[:, pl.ds(512, 256)])
    load("r", hist_r_hbm, hr)
    load("u", hist_t_hbm, ut)
    for part in range(3):
        load(("cs", part), cs_hbm.at[part % 2], cs_wide.at[:, pl.ds(256 * part, 256)])
        load(("hw", part), h_hbm.at[part % 2], h_wide.at[:, pl.ds(512 * part, 512)])
    for a in range(SITES):
        load(("sl", a), self_hbm.at[a, 0], low_chi.at[a])
        load(("cl", a), cross_hbm.at[a, 0], low_chi.at[3 + a])
    for part in range(3):
        load(("ht", part), h_hbm.at[part % 2], h_tall.at[pl.ds(512 * part, 512)])
    load("wb", wb_hbm, w_back)
    top_copies = []
    for a in range(SITES):
        for place, src in ((a, self_hbm), (3 + a, cross_hbm)):
            top_copies.append(
                pltpu.make_async_copy(src.at[a, 1], top_chi.at[place], in_sem.at[counter[0]])
            )
            counter[0] += 1

    @pl.when(leading)
    def _():
        for copy in top_copies:
            copy.start()

    cores = [core, (core + 1) % 2]
    zs = [(site + step) % 4 for step in (2, 1, 3, 0)]

    def distance(place):
        return jnp.where(place < 2, 2 - place, (place + 1) % 4)

    def over_peers(action, sides):
        def step(group, carry):
            chip = ((py + distance(group // 4)) % 4) * 4 + (px + distance(group % 4)) % 4
            for side in sides:
                for z in zs:
                    action(chip * 2 + side, z)
            return carry

        lax.fori_loop(0, 15, step, 0)
        for side in sides:
            for z in zs[:3]:
                action(plane * 2 + side, z)
            if side is cores[1]:
                action(plane * 2 + side, site)
            elif side is not cores[0]:

                @pl.when(core != side)
                def _():
                    action(plane * 2 + side, site)

    barrier = pltpu.get_barrier_semaphore()
    over_peers(
        lambda sl, st: pl.semaphore_signal(
            barrier, inc=1, device_id=(sl, st), device_id_type=MESH
        ),
        cores,
    )

    lane = lax.broadcasted_iota(jnp.int32, (1, 128), 1)
    real_half = lane < 64

    def swap(value):
        return pltpu.roll(value, 64, 1)

    def forward_site(q):
        def chunk(c, carry):
            rows = pl.ds(pl.multiple_of(c * 64, 64), 64)
            indirect = tv[q, rows, :]
            field = indirect - hv[q, rows, :]
            total = jnp.where(field > 0, field, jnp.exp(jnp.minimum(field, 0.0)) - 1.0)
            hv[q, rows, :] = total
            high, low = halves(total - indirect)
            d_b[rows, 0:256] = high
            d_b[rows, 256:512] = high
            d_b[rows, 512:768] = low
            return carry

        lax.fori_loop(0, ROWS // 64, chunk, 0)
        z_f[...] = lax.dot_general(wz_wide[...], d_b[...], NT, preferred_element_type=F32)
        for pair in range(4):
            columns = pl.ds(128 * pair, 128)
            real, imag = z_f[0:128, columns], z_f[128:256, columns]
            first = jnp.where(real_half, real, swap(imag))
            second = jnp.where(real_half, swap(real), imag)
            sent[q, pl.ds(2 * pair, 128, stride=8), :] = first
            sent[q, pl.ds(2 * pair + 1, 128, stride=8), :] = second

    def send_forward(q, side):
        def action(sl, st):
            wave = pl.multiple_of((sl * 4 + st) * 8, 8)
            pltpu.make_async_remote_copy(
                src_ref=sent.at[q, pl.ds(wave, 8)],
                dst_ref=got.at[q, site, pl.ds(pl.multiple_of(slab * 8, 8), 8)],
                send_sem=fsend.at[q],
                recv_sem=frecv.at[q],
                device_id=(sl, st),
                device_id_type=MESH,
            ).start()

        over_peers(action, (side,))

    def keep_own(q):
        got[q, site, pl.ds(pl.multiple_of(slab * 8, 8), 8), :] = sent[
            q, pl.ds(pl.multiple_of(me * 8, 8), 8), :
        ]

    for q in range(SITES):
        copies[("t", q)].wait()
        copies[("p", q)].wait()
        if q == 0:
            for part in range(3):
                copies[f"wz{part}"].wait()
        forward_site(q)

    copies["r"].wait()
    copies["u"].wait()

    def history(c, sums):
        rows = pl.ds(pl.multiple_of(c * 8, 8), 8)
        rs = [hr[i, rows, :] for i in range(HIST)]
        for i in range(HIST):
            ut[i, rows, :] = ut[i, rows, :] + MIXING * rs[i]
        return tuple(s + rs[i] * rs[j] for s, (i, j) in zip(sums, PAIRS))

    zero = jnp.zeros((8, 256), F32)
    past = lax.fori_loop(0, SITES * ROWS // 8, history, (zero,) * len(PAIRS))

    def pack(entries, first):
        row = jnp.zeros((1, 128), F32)
        for place, entry in enumerate(entries):
            folded = entry[:, 0:128] + entry[:, 128:256]
            value = jnp.sum(jnp.sum(folded, axis=0, keepdims=True), axis=1, keepdims=True)
            row = jnp.where(lane == first + place, value, row)
        return row

    past_row = pack(past, 0)

    pl.semaphore_wait(barrier, PEERS)
    for side in range(2):
        for q in range(SITES):
            send_forward(q, side)
    for q in range(SITES):
        keep_own(q)

    for part in range(3):
        copies[("cs", part)].wait()
        copies[("hw", part)].wait()
        copies[("ht", part)].wait()
    copies["wb"].wait()
    for a in range(SITES):
        copies[("sl", a)].wait()
        copies[("cl", a)].wait()

    @pl.when(leading)
    def _():
        for copy in top_copies:
            copy.wait()

    def arrived(sem):
        block = sent.at[0, pl.ds(0, PEERS * 8)]
        pltpu.make_async_copy(block, block, sem).wait()

    def along_y(pick, target, q):
        for s in range(4):
            columns = pl.ds(128 * s, 128)
            one, two = zz_f[0:256, columns], zz_f[256:512, columns]
            high, low = halves(pick(one, two))
            u_b[:, pl.ds(128 * s, 128)] = high
            u_b[:, pl.ds(512 + 128 * s, 128)] = high
            u_b[:, pl.ds(1024 + 128 * s, 128)] = low
        target[q] = lax.dot_general(h_wide[...], u_b[...], NT, preferred_element_type=F32)

    def pick_whole(one, two):
        other = swap(two)
        return one + jnp.where(real_half, other, -other)

    def pick_low(one, two):
        return jnp.where(real_half, one, -swap(two))

    def pick_top(one, two):
        return jnp.where(real_half, swap(one), -two)

    def plane_site(q, carry):
        arrived(frecv.at[q])
        for s in range(4):
            columns = pl.ds(128 * s, 128)
            high, low = halves(got[q, s])
            r_b[0:256, columns] = high
            r_b[256:512, columns] = high
            r_b[512:768, columns] = low
        zz_f[...] = lax.dot_general(cs_wide[...], r_b[...], NN, preferred_element_type=F32)

        @pl.when(leading)
        def _():
            along_y(pick_low, spec, q)
            along_y(pick_top, spec_top, q)

        @pl.when(jnp.logical_not(leading))
        def _():
            along_y(pick_whole, spec, q)

        return carry

    lax.fori_loop(0, SITES, plane_site, 0)

    def combine(chi, field, a, rows, upper):
        total = None
        for g in range(SITES):
            entry = chi[jnp.where(a == g, a, a + g + 2), rows, :]
            term = entry * field[g, upper, :]
            total = term if total is None else total + term
        return total

    def store_mixed(rows, value):
        high, low = halves(value)
        m_b[rows, 0:256] = high
        m_b[rows, 256:512] = high
        m_b[rows, 512:768] = low

    shelf = pl.multiple_of((plane * 4 + site) * 8, 8)

    def back_site(a, carry):
        def mix(c, carry):
            rows = pl.ds(pl.multiple_of(c * 32, 32), 32)
            lower = pl.ds(pl.multiple_of(256 + c * 32, 32), 32)
            real = combine(low_chi, spec, a, rows, rows)
            imag = combine(low_chi, spec, a, rows, lower)

            @pl.when(leading)
            def _():
                top_real = combine(top_chi, spec_top, a, rows, rows)
                top_imag = combine(top_chi, spec_top, a, rows, lower)
                store_mixed(rows, (real - top_imag) * (1.0 / N**3))
                store_mixed(lower, (imag + top_real) * (1.0 / N**3))

            @pl.when(jnp.logical_not(leading))
            def _():
                store_mixed(rows, real * (2.0 / N**3))
                store_mixed(lower, imag * (2.0 / N**3))

            return carry

        lax.fori_loop(0, 8, mix, 0)
        zz_f[...] = lax.dot_general(cs_wide[...], m_b[...], NT, preferred_element_type=F32)
        for block in range(4):
            rows, lower = pl.ds(64 * block, 64), pl.ds(256 + 64 * block, 64)
            real = zz_f[rows, 0:256] - zz_f[lower, 256:512]
            imag = zz_f[rows, 256:512] + zz_f[lower, 0:256]
            for place, value in ((0, real), (256, imag)):
                high, low = halves(value)
                t_b[rows, pl.ds(place, 256)] = high
                t_b[rows, pl.ds(512 + place, 256)] = high
                t_b[rows, pl.ds(1024 + place, 256)] = low
        planes = lax.dot_general(t_b[...], h_tall[...], NN, preferred_element_type=F32)
        for s in range(4):
            back[a, s] = planes[:, 128 * s : 128 * s + 128]

        def action(sl, st):
            pltpu.make_async_remote_copy(
                src_ref=back.at[a, st, pl.ds(pl.multiple_of(sl * 8, 8), 8)],
                dst_ref=home.at[a, core, pl.ds(shelf, 8)],
                send_sem=bsend.at[a],
                recv_sem=brecv.at[core * 3 + a],
                device_id=(sl, st),
                device_id_type=MESH,
            ).start()

        over_peers(action, cores)
        home[a, core, pl.ds(shelf, 8), :] = back[
            a, site, pl.ds(pl.multiple_of(slab * 8, 8), 8), :
        ]
        return carry

    lax.fori_loop(0, SITES, back_site, 0)

    def arrived_home(a, side):
        @pl.when(core == side)
        def _():
            block = sent.at[0, pl.ds(0, 63 * 8)]
            pltpu.make_async_copy(block, block, brecv.at[side * 3 + a]).wait()

        @pl.when(core != side)
        def _():
            block = sent.at[0, pl.ds(0, 64 * 8)]
            pltpu.make_async_copy(block, block, brecv.at[side * 3 + a]).wait()

    def along_z(a, side):
        arrived_home(a, side)
        for pair in range(4):
            lines = jnp.transpose(
                jnp.concatenate(
                    [home[a, side, pl.ds(2 * pair + x, 64, stride=8), :] for x in range(2)], 0
                )
            )
            real, imag = lines[0:64], lines[64:128]
            first = jnp.where(real_half, real, swap(imag))
            second = jnp.where(real_half, swap(real), imag)
            for x, value in ((2 * pair, first), (2 * pair + 1, second)):
                high, low = halves(value)
                rows = pl.ds(64 * x, 64)
                e_b[rows, 0:128] = high
                e_b[rows, 128:256] = high
                e_b[rows, 256:384] = low
        y_f[...] = lax.dot_general(e_b[...], w_back[side], NN, preferred_element_type=F32)

    def home_first(a, carry):
        along_z(a, 0)

        def chunk(c, carry):
            rows = pl.ds(pl.multiple_of(c * 32, 32), 32)
            hv[a, rows, :] = y_f[rows, :] - hv[a, rows, :]
            return carry

        return lax.fori_loop(0, ROWS // 32, chunk, carry)

    lax.fori_loop(0, SITES, home_first, 0)

    def home_second(a, sums):
        along_z(a, 1)

        def chunk(c, sums):
            rows = pl.ds(pl.multiple_of(c * 8, 8), 8)
            latest = y_f[rows, :] + hv[a, rows, :]
            last_ref[a, rows, :] = latest
            tv[a, rows, :] = tv[a, rows, :] + MIXING * latest
            offset = pl.ds(pl.multiple_of(a * ROWS + c * 8, 8), 8)
            new = [s + hr[i, offset, :] * latest for i, s in enumerate(sums[:HIST])]
            return tuple(new) + (sums[HIST] + latest * latest,)

        return lax.fori_loop(0, ROWS // 8, chunk, sums, unroll=2)

    newest = lax.fori_loop(0, SITES, home_second, (zero,) * (HIST + 1))

    row = past_row + pack(newest, len(PAIRS))
    g_row[0:1, :] = row

    def send_row(sl, st):
        pltpu.make_async_remote_copy(
            src_ref=g_row.at[pl.ds(0, 1)],
            dst_ref=g_all.at[pl.ds(me, 1)],
            send_sem=gsend,
            recv_sem=grecv,
            device_id=(sl, st),
            device_id_type=MESH,
        ).start()

    over_peers(send_row, cores)
    g_all[pl.ds(me, 1), :] = row

    def wait_rows(sem):
        block = g_all.at[pl.ds(0, PEERS)]
        pltpu.make_async_copy(block, block, sem).wait()

    wait_rows(grecv)
    whole = jnp.sum(g_all[...], axis=0, keepdims=True)

    gram = [[None] * (HIST + 1) for i in range(HIST + 1)]
    for index, (i, j) in enumerate(PAIRS + [(i, HIST) for i in range(HIST + 1)]):
        value = jnp.sum(jnp.where(lane == index, whole, 0.0), axis=1, keepdims=True)
        gram[i][j] = gram[j][i] = jnp.broadcast_to(value, (1, 128))
    weights = [
        jnp.broadcast_to(jnp.concatenate([weight, weight], 1), (8, 256))
        for weight in solve_weights(gram)
    ]

    for a in range(SITES):

        def finish(c, carry):
            rows = pl.ds(pl.multiple_of(c * 8, 8), 8)
            offset = pl.ds(pl.multiple_of(a * ROWS + c * 8, 8), 8)
            value = weights[0] * ut[0, offset, :]
            for i in range(1, HIST):
                value = value + weights[i] * ut[i, offset, :]
            next_ref[a, rows, :] = value + weights[HIST] * tv[a, rows, :]
            return carry

        lax.fori_loop(0, ROWS // 8, finish, 0, unroll=4)

    for q in range(SITES):
        arrived(fsend.at[q])
        arrived(bsend.at[q])
    wait_rows(gsend)


def step(potential, t_now, hist_t, hist_r, chi_self, chi_cross):
    flat = (SITES, ROWS, N)
    wz, cs, hh, wb = tables()
    vm = pltpu.VMEM
    field = pltpu.VMEM(flat, F32)
    scratch = [
        vm(flat, F32), vm(flat, F32),
        vm((HIST, SITES * ROWS, N), F32), vm((HIST, SITES * ROWS, N), F32),
        vm((6, N, N), F32), vm((6, N, N), F32),
        vm((256, 768), BF16), vm((2, 384, 256), BF16), vm((512, 768), BF16),
        vm((512, 1536), BF16), vm((1536, 512), BF16),
        vm((SITES, 1024, 128), F32), vm((SITES, 4, 256, 128), F32),
        vm((SITES, 512, 256), F32), vm((SITES, 512, 256), F32),
        vm((SITES, 4, 256, 128), F32), vm((SITES, 2, 512, 128), F32),
        vm((512, 768), BF16), vm((256, 512), F32), vm((768, 512), BF16),
        vm((512, 512), F32), vm((256, 1536), BF16), vm((512, 768), BF16),
        vm((256, 1536), BF16), vm((512, 384), BF16), vm((512, 256), F32),
        vm((8, 128), F32), vm((128, 128), F32),
        pltpu.SemaphoreType.DMA((40,)),
        pltpu.SemaphoreType.DMA((3,)), pltpu.SemaphoreType.DMA((3,)),
        pltpu.SemaphoreType.DMA((3,)), pltpu.SemaphoreType.DMA((6,)),
        pltpu.SemaphoreType.DMA, pltpu.SemaphoreType.DMA,
    ]
    anywhere = pl.BlockSpec(memory_space=pltpu.HBM)
    t_next, residual = pl.pallas_call(
        kernel,
        out_shape=(field, field),
        in_specs=[anywhere] * 10,
        out_specs=(pl.BlockSpec(memory_space=pltpu.VMEM),) * 2,
        scratch_shapes=scratch,
        compiler_params=pltpu.CompilerParams(
            collective_id=0, has_side_effects=True, vmem_limit_bytes=60 * 1024 * 1024 + 512 * 1024
        ),
    )(
        potential.reshape(flat),
        t_now.reshape(flat),
        hist_t.reshape(HIST, SITES * ROWS, N),
        hist_r.reshape(HIST, SITES * ROWS, N),
        chi_self,
        chi_cross,
        jnp.asarray(wz),
        jnp.asarray(cs),
        jnp.asarray(hh),
        jnp.asarray(wb),
    )
    return t_next.reshape(t_now.shape), residual.reshape(t_now.shape)


def solution(mesh):
    field = P(None, "slab", "site", None)
    past = P(None, None, "slab", "site", None)
    chi = P(None, ("slab", "site"), None, None)
    return jax.shard_map(
        step,
        mesh=mesh,
        in_specs=(field, field, past, past, chi, chi),
        out_specs=(field, field),
        check_vma=False,
    )
```

```python
import functools
import math

import jax
import jax.numpy as jnp
import numpy as np
from jax import lax
from jax.experimental import pallas as pl
from jax.experimental.pallas import tpu as pltpu
from jax.sharding import PartitionSpec as P

N = 256
HALF = N // 2
SITES = 3
HIST = 4
MIXING = 0.5
MESH = pl.DeviceIdType.MESH
F32 = jnp.float32
BF16 = jnp.bfloat16

ROWS = 512
PEERS = 127

NT = (((1,), (1,)), ((), ()))
NN = (((1,), (0,)), ((), ()))


def split_table(table):
    high = table.astype(np.float32).astype(jnp.bfloat16)
    low = (table - high.astype(np.float64)).astype(np.float32).astype(jnp.bfloat16)
    return np.stack([high, low])


def tables():
    index = np.arange(N)
    angles = (index[:, None] * index[None, :] % N) * (2.0 * math.pi / N)
    cosine, sine = np.cos(angles), np.sin(angles)
    imag_rows = -sine[:HALF].copy()
    imag_rows[0] = 1.0 - 2.0 * (index % 2)
    along_z = np.concatenate([cosine[:HALF], imag_rows], 0)
    along_x = np.concatenate([cosine, sine], 0)
    blocks = np.stack([cosine.reshape(N, 4, 64), sine.reshape(N, 4, 64)], 2).reshape(N, 512)
    turned = np.stack([-sine.reshape(N, 4, 64), cosine.reshape(N, 4, 64)], 2).reshape(N, 512)
    along_y = np.concatenate([blocks, turned], 0)
    waves = np.arange(HALF).reshape(16, 2, 4)
    cuts = [split_table(along_z[np.concatenate([w, w + HALF])]) for w in (waves[:, c].ravel() for c in (0, 1))]
    from_z = np.stack([np.concatenate([cut[0], cut[1], cut[0]], 0) for cut in cuts])
    return split_table(along_z), split_table(along_x), split_table(along_y), from_z


def halves(value):
    high = value.astype(BF16)
    low = (value - high.astype(F32)).astype(BF16)
    return high, low


def solve_weights(gram):
    count = HIST + 1
    factor = [[None] * count for member in range(count)]
    for column in range(count):
        diagonal_sum = gram[column][column]
        for inner in range(column):
            diagonal_sum = diagonal_sum - factor[column][inner] * factor[column][inner]
        factor[column][column] = jnp.sqrt(diagonal_sum)
        for row in range(column + 1, count):
            entry = gram[row][column]
            for inner in range(column):
                entry = entry - factor[row][inner] * factor[column][inner]
            factor[row][column] = entry / factor[column][column]
    middle = []
    for row in range(count):
        entry = jnp.ones_like(gram[0][0])
        for inner in range(row):
            entry = entry - factor[row][inner] * middle[inner]
        middle.append(entry / factor[row][row])
    weights = [None] * count
    for row in range(count - 1, -1, -1):
        entry = middle[row]
        for inner in range(row + 1, count):
            entry = entry - factor[inner][row] * weights[inner]
        weights[row] = entry / factor[row][row]
    total = weights[0]
    for row in range(1, count):
        total = total + weights[row]
    return [weight / total for weight in weights]


PAIRS = [(i, j) for i in range(HIST) for j in range(i, HIST)]


def kernel(
    pot_hbm, t_hbm, hist_t_hbm, hist_r_hbm, self_hbm, cross_hbm, wz_hbm, cs_hbm, h_hbm, wb_hbm,
    weight_ref, ut, tv, last_ref,
    hv, hr, low_chi, top_chi,
    wz_wide, w_back, cs_wide, h_wide, h_tall,
    sent, got, spec, spec_top, back, home,
    d_b, z_f, r_b, zz_f, u_b, m_b, t_b, e_b, y_f,
    g_row, g_all,
    in_sem, fsend, frecv, bsend, brecv, gsend, grecv,
):
    slab = lax.axis_index("slab")
    site = lax.axis_index("site")
    plane = slab // 2
    py, px, core = plane // 4, plane % 4, slab % 2
    me = slab * 4 + site
    leading = me == 0

    counter = [0]
    copies = {}

    def load(name, src, dst):
        copy = pltpu.make_async_copy(src, dst, in_sem.at[counter[0]])
        counter[0] += 1
        copies[name] = copy
        copy.start()

    for q in range(SITES):
        load(("t", q), t_hbm.at[q], tv.at[q])
        load(("p", q), pot_hbm.at[q], hv.at[q])
        if q == 0:
            load("wz0", wz_hbm.at[0], wz_wide.at[:, pl.ds(0, 256)])
            load("wz1", wz_hbm.at[1], wz_wide.at[:, pl.ds(256, 256)])
            load("wz2", wz_hbm.at[0], wz_wide.at[:, pl.ds(512, 256)])
    cores = [core, (core + 1) % 2]
    zs = [(site + step) % 4 for step in (2, 1, 3, 0)]

    def distance(place):
        return jnp.where(place < 2, 2 - place, (place + 1) % 4)

    def over_peers(action, sides):
        def step(group, carry):
            chip = ((py + distance(group // 4)) % 4) * 4 + (px + distance(group % 4)) % 4
            for side in sides:
                for z in zs:
                    action(chip * 2 + side, z)
            return carry

        lax.fori_loop(0, 15, step, 0)
        for side in sides:
            for z in zs[:3]:
                action(plane * 2 + side, z)
            if side is cores[1]:
                action(plane * 2 + side, site)
            elif side is not cores[0]:

                @pl.when(core != side)
                def _():
                    action(plane * 2 + side, site)

    barrier = pltpu.get_barrier_semaphore()
    over_peers(
        lambda sl, st: pl.semaphore_signal(
            barrier, inc=1, device_id=(sl, st), device_id_type=MESH
        ),
        cores,
    )

    lane = lax.broadcasted_iota(jnp.int32, (1, 128), 1)
    real_half = lane < 64

    def swap(value):
        return pltpu.roll(value, 64, 1)

    def forward_site(q):
        def chunk(c, carry):
            rows = pl.ds(pl.multiple_of(c * 64, 64), 64)
            indirect = tv[q, rows, :]
            field = indirect - hv[q, rows, :]
            total = jnp.where(field > 0, field, jnp.exp(jnp.minimum(field, 0.0)) - 1.0)
            hv[q, rows, :] = total
            high, low = halves(total - indirect)
            d_b[rows, 0:256] = high
            d_b[rows, 256:512] = high
            d_b[rows, 512:768] = low
            return carry

        lax.fori_loop(0, ROWS // 64, chunk, 0)
        z_f[...] = lax.dot_general(wz_wide[...], d_b[...], NT, preferred_element_type=F32)
        for pair in range(4):
            columns = pl.ds(128 * pair, 128)
            real, imag = z_f[0:128, columns], z_f[128:256, columns]
            first = jnp.where(real_half, real, swap(imag))
            second = jnp.where(real_half, swap(real), imag)
            sent[q, pl.ds(2 * pair, 128, stride=8), :] = first
            sent[q, pl.ds(2 * pair + 1, 128, stride=8), :] = second

    def send_forward(q, side):
        def action(sl, st):
            wave = pl.multiple_of((sl * 4 + st) * 8, 8)
            pltpu.make_async_remote_copy(
                src_ref=sent.at[q, pl.ds(wave, 8)],
                dst_ref=got.at[q, site, pl.ds(pl.multiple_of(slab * 8, 8), 8)],
                send_sem=fsend.at[q],
                recv_sem=frecv.at[q],
                device_id=(sl, st),
                device_id_type=MESH,
            ).start()

        over_peers(action, (side,))

    def keep_own(q):
        got[q, site, pl.ds(pl.multiple_of(slab * 8, 8), 8), :] = sent[
            q, pl.ds(pl.multiple_of(me * 8, 8), 8), :
        ]

    for q in range(SITES):
        copies[("t", q)].wait()
        copies[("p", q)].wait()
        if q == 0:
            for part in range(3):
                copies[f"wz{part}"].wait()
            load("r", hist_r_hbm, hr)
            load("u", hist_t_hbm, ut)
            for part in range(3):
                load(("cs", part), cs_hbm.at[part % 2], cs_wide.at[:, pl.ds(256 * part, 256)])
                load(("hw", part), h_hbm.at[part % 2], h_wide.at[:, pl.ds(512 * part, 512)])
            for a in range(SITES):
                load(("sl", a), self_hbm.at[a, 0], low_chi.at[a])
                load(("cl", a), cross_hbm.at[a, 0], low_chi.at[3 + a])
            for part in range(3):
                load(("ht", part), h_hbm.at[part % 2], h_tall.at[pl.ds(512 * part, 512)])
            load("wb", wb_hbm, w_back)
            top_copies = []
            for a in range(SITES):
                for place, src in ((a, self_hbm), (3 + a, cross_hbm)):
                    top_copies.append(
                        pltpu.make_async_copy(src.at[a, 1], top_chi.at[place], in_sem.at[counter[0]])
                    )
                    counter[0] += 1

            @pl.when(leading)
            def _():
                for copy in top_copies:
                    copy.start()

        forward_site(q)
        if q == 0:
            pl.semaphore_wait(barrier, PEERS)
        send_forward(q, 0)
    for q in range(SITES):
        send_forward(q, 1)
        keep_own(q)

    copies["r"].wait()
    copies["u"].wait()

    def history(c, sums):
        rows = pl.ds(pl.multiple_of(c * 8, 8), 8)
        rs = [hr[i, rows, :] for i in range(HIST)]
        for i in range(HIST):
            ut[i, rows, :] = ut[i, rows, :] + MIXING * rs[i]
        return tuple(s + rs[i] * rs[j] for s, (i, j) in zip(sums, PAIRS))

    zero = jnp.zeros((8, 256), F32)
    past = lax.fori_loop(0, SITES * ROWS // 8, history, (zero,) * len(PAIRS))

    def pack(entries, first):
        row = jnp.zeros((1, 128), F32)
        for place, entry in enumerate(entries):
            folded = entry[:, 0:128] + entry[:, 128:256]
            value = jnp.sum(jnp.sum(folded, axis=0, keepdims=True), axis=1, keepdims=True)
            row = jnp.where(lane == first + place, value, row)
        return row

    past_row = pack(past, 0)

    for part in range(3):
        copies[("cs", part)].wait()
        copies[("hw", part)].wait()
        copies[("ht", part)].wait()
    copies["wb"].wait()
    for a in range(SITES):
        copies[("sl", a)].wait()
        copies[("cl", a)].wait()

    @pl.when(leading)
    def _():
        for copy in top_copies:
            copy.wait()

    def arrived(sem):
        block = sent.at[0, pl.ds(0, PEERS * 8)]
        pltpu.make_async_copy(block, block, sem).wait()

    def along_y(pick, target, q):
        for s in range(4):
            columns = pl.ds(128 * s, 128)
            one, two = zz_f[0:256, columns], zz_f[256:512, columns]
            high, low = halves(pick(one, two))
            u_b[:, pl.ds(128 * s, 128)] = high
            u_b[:, pl.ds(512 + 128 * s, 128)] = high
            u_b[:, pl.ds(1024 + 128 * s, 128)] = low
        target[q] = lax.dot_general(h_wide[...], u_b[...], NT, preferred_element_type=F32)

    def pick_whole(one, two):
        other = swap(two)
        return one + jnp.where(real_half, other, -other)

    def pick_low(one, two):
        return jnp.where(real_half, one, -swap(two))

    def pick_top(one, two):
        return jnp.where(real_half, swap(one), -two)

    def plane_site(q, carry):
        arrived(frecv.at[q])
        for s in range(4):
            columns = pl.ds(128 * s, 128)
            high, low = halves(got[q, s])
            r_b[0:256, columns] = high
            r_b[256:512, columns] = high
            r_b[512:768, columns] = low
        zz_f[...] = lax.dot_general(cs_wide[...], r_b[...], NN, preferred_element_type=F32)

        @pl.when(leading)
        def _():
            along_y(pick_low, spec, q)
            along_y(pick_top, spec_top, q)

        @pl.when(jnp.logical_not(leading))
        def _():
            along_y(pick_whole, spec, q)

        return carry

    lax.fori_loop(0, SITES, plane_site, 0)

    def combine(chi, field, a, rows, upper):
        total = None
        for g in range(SITES):
            entry = chi[jnp.where(a == g, a, a + g + 2), rows, :]
            term = entry * field[g, upper, :]
            total = term if total is None else total + term
        return total

    def store_mixed(rows, value):
        high, low = halves(value)
        m_b[rows, 0:256] = high
        m_b[rows, 256:512] = high
        m_b[rows, 512:768] = low

    shelf = pl.multiple_of((plane * 4 + site) * 8, 8)

    def back_site(a, carry):
        def mix(c, carry):
            rows = pl.ds(pl.multiple_of(c * 32, 32), 32)
            lower = pl.ds(pl.multiple_of(256 + c * 32, 32), 32)
            real = combine(low_chi, spec, a, rows, rows)
            imag = combine(low_chi, spec, a, rows, lower)

            @pl.when(leading)
            def _():
                top_real = combine(top_chi, spec_top, a, rows, rows)
                top_imag = combine(top_chi, spec_top, a, rows, lower)
                store_mixed(rows, (real - top_imag) * (1.0 / N**3))
                store_mixed(lower, (imag + top_real) * (1.0 / N**3))

            @pl.when(jnp.logical_not(leading))
            def _():
                store_mixed(rows, real * (2.0 / N**3))
                store_mixed(lower, imag * (2.0 / N**3))

            return carry

        lax.fori_loop(0, 8, mix, 0)
        zz_f[...] = lax.dot_general(cs_wide[...], m_b[...], NT, preferred_element_type=F32)
        for block in range(4):
            rows, lower = pl.ds(64 * block, 64), pl.ds(256 + 64 * block, 64)
            real = zz_f[rows, 0:256] - zz_f[lower, 256:512]
            imag = zz_f[rows, 256:512] + zz_f[lower, 0:256]
            for place, value in ((0, real), (256, imag)):
                high, low = halves(value)
                t_b[rows, pl.ds(place, 256)] = high
                t_b[rows, pl.ds(512 + place, 256)] = high
                t_b[rows, pl.ds(1024 + place, 256)] = low
        planes = lax.dot_general(t_b[...], h_tall[...], NN, preferred_element_type=F32)
        for s in range(4):
            back[a, s] = planes[:, 128 * s : 128 * s + 128]

        def action(sl, st):
            pltpu.make_async_remote_copy(
                src_ref=back.at[a, st, pl.ds(pl.multiple_of(sl * 8, 8), 8)],
                dst_ref=home.at[a, core, pl.ds(shelf, 8)],
                send_sem=bsend.at[a],
                recv_sem=brecv.at[core * 3 + a],
                device_id=(sl, st),
                device_id_type=MESH,
            ).start()

        over_peers(action, cores)
        home[a, core, pl.ds(shelf, 8), :] = back[
            a, site, pl.ds(pl.multiple_of(slab * 8, 8), 8), :
        ]
        return carry

    lax.fori_loop(0, SITES, back_site, 0)

    def arrived_home(a, side):
        @pl.when(core == side)
        def _():
            block = sent.at[0, pl.ds(0, 63 * 8)]
            pltpu.make_async_copy(block, block, brecv.at[side * 3 + a]).wait()

        @pl.when(core != side)
        def _():
            block = sent.at[0, pl.ds(0, 64 * 8)]
            pltpu.make_async_copy(block, block, brecv.at[side * 3 + a]).wait()

    def along_z(a, side):
        arrived_home(a, side)
        for pair in range(4):
            lines = jnp.transpose(
                jnp.concatenate(
                    [home[a, side, pl.ds(2 * pair + x, 64, stride=8), :] for x in range(2)], 0
                )
            )
            real, imag = lines[0:64], lines[64:128]
            first = jnp.where(real_half, real, swap(imag))
            second = jnp.where(real_half, swap(real), imag)
            for x, value in ((2 * pair, first), (2 * pair + 1, second)):
                high, low = halves(value)
                rows = pl.ds(64 * x, 64)
                e_b[rows, 0:128] = high
                e_b[rows, 128:256] = high
                e_b[rows, 256:384] = low
        y_f[...] = lax.dot_general(e_b[...], w_back[side], NN, preferred_element_type=F32)

    def home_first(a, carry):
        along_z(a, 0)

        def chunk(c, carry):
            rows = pl.ds(pl.multiple_of(c * 32, 32), 32)
            hv[a, rows, :] = y_f[rows, :] - hv[a, rows, :]
            return carry

        return lax.fori_loop(0, ROWS // 32, chunk, carry)

    lax.fori_loop(0, SITES, home_first, 0)

    def home_second(a, sums):
        along_z(a, 1)

        def chunk(c, sums):
            rows = pl.ds(pl.multiple_of(c * 8, 8), 8)
            latest = y_f[rows, :] + hv[a, rows, :]
            last_ref[a, rows, :] = latest
            tv[a, rows, :] = tv[a, rows, :] + MIXING * latest
            offset = pl.ds(pl.multiple_of(a * ROWS + c * 8, 8), 8)
            new = [s + hr[i, offset, :] * latest for i, s in enumerate(sums[:HIST])]
            return tuple(new) + (sums[HIST] + latest * latest,)

        return lax.fori_loop(0, ROWS // 8, chunk, sums, unroll=2)

    newest = lax.fori_loop(0, SITES, home_second, (zero,) * (HIST + 1))

    row = past_row + pack(newest, len(PAIRS))
    g_row[0:1, :] = row

    def send_row(sl, st):
        pltpu.make_async_remote_copy(
            src_ref=g_row.at[pl.ds(0, 1)],
            dst_ref=g_all.at[pl.ds(me, 1)],
            send_sem=gsend,
            recv_sem=grecv,
            device_id=(sl, st),
            device_id_type=MESH,
        ).start()

    over_peers(send_row, cores)
    g_all[pl.ds(me, 1), :] = row

    def wait_rows(sem):
        block = g_all.at[pl.ds(0, PEERS)]
        pltpu.make_async_copy(block, block, sem).wait()

    wait_rows(grecv)
    whole = jnp.sum(g_all[...], axis=0, keepdims=True)

    gram = [[None] * (HIST + 1) for i in range(HIST + 1)]
    for index, (i, j) in enumerate(PAIRS + [(i, HIST) for i in range(HIST + 1)]):
        value = jnp.sum(jnp.where(lane == index, whole, 0.0), axis=1, keepdims=True)
        gram[i][j] = gram[j][i] = jnp.broadcast_to(value, (1, 128))
    for i, weight in enumerate(solve_weights(gram)):
        weight_ref[i : i + 1, :] = weight

    for q in range(SITES):
        arrived(fsend.at[q])
        arrived(bsend.at[q])
    wait_rows(gsend)


def last_kernel(weight_ref, ut, tv, last_vmem, next_hbm, last_hbm, res, sem):
    pltpu.make_async_copy(last_vmem, last_hbm, sem.at[SITES]).start()
    weights = []
    for i in range(HIST + 1):
        weight = weight_ref[i : i + 1, :]
        weights.append(jnp.broadcast_to(jnp.concatenate([weight, weight], 1), (8, 256)))
    for a in range(SITES):

        def finish(c, carry):
            rows = pl.ds(pl.multiple_of(c * 8, 8), 8)
            offset = pl.ds(pl.multiple_of(a * ROWS + c * 8, 8), 8)
            value = weights[0] * ut[0, offset, :]
            for i in range(1, HIST):
                value = value + weights[i] * ut[i, offset, :]
            res[a, rows, :] = value + weights[HIST] * tv[a, rows, :]
            return carry

        lax.fori_loop(0, ROWS // 8, finish, 0, unroll=4)
        pltpu.make_async_copy(res.at[a], next_hbm.at[a], sem.at[a]).start()
    for a in range(SITES):
        pltpu.make_async_copy(res.at[a], next_hbm.at[a], sem.at[a]).wait()
    pltpu.make_async_copy(last_vmem, last_hbm, sem.at[SITES]).wait()


def step(potential, t_now, hist_t, hist_r, chi_self, chi_cross):
    flat = (SITES, ROWS, N)
    wz, cs, hh, wb = tables()
    vm = pltpu.VMEM
    field = pltpu.VMEM(flat, F32)
    whole = pl.BlockSpec(memory_space=pltpu.VMEM)
    scratch = [
        vm(flat, F32), vm((HIST, SITES * ROWS, N), F32),
        vm((6, N, N), F32), vm((6, N, N), F32),
        vm((256, 768), BF16), vm((2, 384, 256), BF16), vm((512, 768), BF16),
        vm((512, 1536), BF16), vm((1536, 512), BF16),
        vm((SITES, 1024, 128), F32), vm((SITES, 4, 256, 128), F32),
        vm((SITES, 512, 256), F32), vm((SITES, 512, 256), F32),
        vm((SITES, 4, 256, 128), F32), vm((SITES, 2, 512, 128), F32),
        vm((512, 768), BF16), vm((256, 512), F32), vm((768, 512), BF16),
        vm((512, 512), F32), vm((256, 1536), BF16), vm((512, 768), BF16),
        vm((256, 1536), BF16), vm((512, 384), BF16), vm((512, 256), F32),
        vm((8, 128), F32), vm((128, 128), F32),
        pltpu.SemaphoreType.DMA((40,)),
        pltpu.SemaphoreType.DMA((3,)), pltpu.SemaphoreType.DMA((3,)),
        pltpu.SemaphoreType.DMA((3,)), pltpu.SemaphoreType.DMA((6,)),
        pltpu.SemaphoreType.DMA, pltpu.SemaphoreType.DMA,
    ]
    anywhere = pl.BlockSpec(memory_space=pltpu.HBM)
    inner = pl.pallas_call(
        kernel,
        out_shape=(vm((8, 128), F32), vm((HIST, SITES * ROWS, N), F32), field, field),
        in_specs=[anywhere] * 10,
        out_specs=(whole,) * 4,
        scratch_shapes=scratch,
        compiler_params=pltpu.CompilerParams(
            collective_id=0, has_side_effects=True, vmem_limit_bytes=54 * 1024 * 1024
        ),
    )(
        potential.reshape(flat),
        t_now.reshape(flat),
        hist_t.reshape(HIST, SITES * ROWS, N),
        hist_r.reshape(HIST, SITES * ROWS, N),
        chi_self,
        chi_cross,
        jnp.asarray(wz),
        jnp.asarray(cs),
        jnp.asarray(hh),
        jnp.asarray(wb),
    )
    outer = jax.ShapeDtypeStruct(flat, F32)
    t_next, residual = pl.pallas_call(
        last_kernel,
        out_shape=(outer, outer),
        in_specs=[whole] * 4,
        out_specs=(anywhere, anywhere),
        scratch_shapes=[vm(flat, F32), pltpu.SemaphoreType.DMA((SITES + 1,))],
        compiler_params=pltpu.CompilerParams(vmem_limit_bytes=16 * 1024 * 1024),
    )(*inner)
    return t_next.reshape(t_now.shape), residual.reshape(t_now.shape)


def solution(mesh):
    field = P(None, "slab", "site", None)
    past = P(None, None, "slab", "site", None)
    chi = P(None, ("slab", "site"), None, None)
    return jax.shard_map(
        step,
        mesh=mesh,
        in_specs=(field, field, past, past, chi, chi),
        out_specs=(field, field),
        check_vma=False,
    )
```

```python
import functools
import math

import jax
import jax.numpy as jnp
import numpy as np
from jax import lax
from jax.experimental import pallas as pl
from jax.experimental.pallas import tpu as pltpu
from jax.sharding import PartitionSpec as P

N = 256
HALF = N // 2
SITES = 3
HIST = 4
MIXING = 0.5
MESH = pl.DeviceIdType.MESH
F32 = jnp.float32
BF16 = jnp.bfloat16

ROWS = 512
PEERS = 127

NT = (((1,), (1,)), ((), ()))
NN = (((1,), (0,)), ((), ()))


def split_table(table):
    high = table.astype(np.float32).astype(jnp.bfloat16)
    low = (table - high.astype(np.float64)).astype(np.float32).astype(jnp.bfloat16)
    return np.stack([high, low])


def tables():
    index = np.arange(N)
    angles = (index[:, None] * index[None, :] % N) * (2.0 * math.pi / N)
    cosine, sine = np.cos(angles), np.sin(angles)
    imag_rows = -sine[:HALF].copy()
    imag_rows[0] = 1.0 - 2.0 * (index % 2)
    along_z = np.concatenate([cosine[:HALF], imag_rows], 0)
    along_x = np.concatenate([cosine, sine], 0)
    blocks = np.stack([cosine.reshape(N, 4, 64), sine.reshape(N, 4, 64)], 2).reshape(N, 512)
    turned = np.stack([-sine.reshape(N, 4, 64), cosine.reshape(N, 4, 64)], 2).reshape(N, 512)
    along_y = np.concatenate([blocks, turned], 0)
    waves = np.arange(HALF).reshape(16, 2, 4)
    cuts = [split_table(along_z[np.concatenate([w, w + HALF])]) for w in (waves[:, c].ravel() for c in (0, 1))]
    from_z = np.stack([np.concatenate([cut[0], cut[1], cut[0]], 0) for cut in cuts])
    return split_table(along_z), split_table(along_x), split_table(along_y), from_z


def halves(value):
    high = value.astype(BF16)
    low = (value - high.astype(F32)).astype(BF16)
    return high, low


def solve_weights(gram):
    count = HIST + 1
    factor = [[None] * count for member in range(count)]
    for column in range(count):
        diagonal_sum = gram[column][column]
        for inner in range(column):
            diagonal_sum = diagonal_sum - factor[column][inner] * factor[column][inner]
        factor[column][column] = jnp.sqrt(diagonal_sum)
        for row in range(column + 1, count):
            entry = gram[row][column]
            for inner in range(column):
                entry = entry - factor[row][inner] * factor[column][inner]
            factor[row][column] = entry / factor[column][column]
    middle = []
    for row in range(count):
        entry = jnp.ones_like(gram[0][0])
        for inner in range(row):
            entry = entry - factor[row][inner] * middle[inner]
        middle.append(entry / factor[row][row])
    weights = [None] * count
    for row in range(count - 1, -1, -1):
        entry = middle[row]
        for inner in range(row + 1, count):
            entry = entry - factor[inner][row] * weights[inner]
        weights[row] = entry / factor[row][row]
    total = weights[0]
    for row in range(1, count):
        total = total + weights[row]
    return [weight / total for weight in weights]


PAIRS = [(i, j) for i in range(HIST) for j in range(i, HIST)]


def kernel(
    pot_hbm, t_hbm, hist_t_hbm, hist_r_hbm, self_hbm, cross_hbm, wz_hbm, cs_hbm, h_hbm, wb_hbm,
    weight_ref, ut, tv, last_ref,
    hv, hr, low_chi, top_chi,
    wz_wide, w_back, cs_wide, h_wide, h_tall,
    sent, got, spec, spec_top, back, home,
    d_b, z_f, r_b, zz_f, u_b, m_b, t_b, e_b, y_f,
    g_row, g_all,
    in_sem, fsend, frecv, bsend, brecv, gsend, grecv,
):
    slab = lax.axis_index("slab")
    site = lax.axis_index("site")
    plane = slab // 2
    py, px, core = plane // 4, plane % 4, slab % 2
    me = slab * 4 + site
    leading = me == 0

    counter = [0]
    copies = {}

    def load(name, src, dst):
        copy = pltpu.make_async_copy(src, dst, in_sem.at[counter[0]])
        counter[0] += 1
        copies[name] = copy
        copy.start()

    for q in range(SITES):
        load(("t", q), t_hbm.at[q], tv.at[q])
        load(("p", q), pot_hbm.at[q], hv.at[q])
        if q == 0:
            load("wz0", wz_hbm.at[0], wz_wide.at[:, pl.ds(0, 256)])
            load("wz1", wz_hbm.at[1], wz_wide.at[:, pl.ds(256, 256)])
            load("wz2", wz_hbm.at[0], wz_wide.at[:, pl.ds(512, 256)])
    cores = [core, (core + 1) % 2]
    zs = [(site + step) % 4 for step in (2, 1, 3, 0)]

    def distance(place):
        return jnp.where(place < 2, 2 - place, (place + 1) % 4)

    def over_peers(action, sides):
        def step(group, carry):
            chip = ((py + distance(group // 4)) % 4) * 4 + (px + distance(group % 4)) % 4
            for side in sides:
                for z in zs:
                    action(chip * 2 + side, z)
            return carry

        lax.fori_loop(0, 15, step, 0)
        for side in sides:
            for z in zs[:3]:
                action(plane * 2 + side, z)
            if side is cores[1]:
                action(plane * 2 + side, site)
            elif side is not cores[0]:

                @pl.when(core != side)
                def _():
                    action(plane * 2 + side, site)

    barrier = pltpu.get_barrier_semaphore()
    over_peers(
        lambda sl, st: pl.semaphore_signal(
            barrier, inc=1, device_id=(sl, st), device_id_type=MESH
        ),
        cores,
    )

    lane = lax.broadcasted_iota(jnp.int32, (1, 128), 1)
    real_half = lane < 64

    def swap(value):
        return pltpu.roll(value, 64, 1)

    def forward_site(q):
        def chunk(c, carry):
            rows = pl.ds(pl.multiple_of(c * 64, 64), 64)
            indirect = tv[q, rows, :]
            field = indirect - hv[q, rows, :]
            total = jnp.where(field > 0, field, jnp.exp(jnp.minimum(field, 0.0)) - 1.0)
            hv[q, rows, :] = total
            high, low = halves(total - indirect)
            d_b[rows, 0:256] = high
            d_b[rows, 256:512] = high
            d_b[rows, 512:768] = low
            return carry

        lax.fori_loop(0, ROWS // 64, chunk, 0)
        z_f[...] = lax.dot_general(wz_wide[...], d_b[...], NT, preferred_element_type=F32)
        for pair in range(4):
            columns = pl.ds(128 * pair, 128)
            real, imag = z_f[0:128, columns], z_f[128:256, columns]
            first = jnp.where(real_half, real, swap(imag))
            second = jnp.where(real_half, swap(real), imag)
            sent[q, pl.ds(2 * pair, 128, stride=8), :] = first
            sent[q, pl.ds(2 * pair + 1, 128, stride=8), :] = second

    def send_forward(q, side):
        def action(sl, st):
            wave = pl.multiple_of((sl * 4 + st) * 8, 8)
            pltpu.make_async_remote_copy(
                src_ref=sent.at[q, pl.ds(wave, 8)],
                dst_ref=got.at[q, site, pl.ds(pl.multiple_of(slab * 8, 8), 8)],
                send_sem=fsend.at[q],
                recv_sem=frecv.at[q],
                device_id=(sl, st),
                device_id_type=MESH,
            ).start()

        over_peers(action, (side,))

    def keep_own(q):
        got[q, site, pl.ds(pl.multiple_of(slab * 8, 8), 8), :] = sent[
            q, pl.ds(pl.multiple_of(me * 8, 8), 8), :
        ]

    for q in range(SITES):
        copies[("t", q)].wait()
        copies[("p", q)].wait()
        if q == 0:
            for part in range(3):
                copies[f"wz{part}"].wait()
            load("r", hist_r_hbm, hr)
            load("u", hist_t_hbm, ut)
            for part in range(3):
                load(("cs", part), cs_hbm.at[part % 2], cs_wide.at[:, pl.ds(256 * part, 256)])
                load(("hw", part), h_hbm.at[part % 2], h_wide.at[:, pl.ds(512 * part, 512)])
            for a in range(SITES):
                load(("sl", a), self_hbm.at[a, 0], low_chi.at[a])
                load(("cl", a), cross_hbm.at[a, 0], low_chi.at[3 + a])
            for part in range(3):
                load(("ht", part), h_hbm.at[part % 2], h_tall.at[pl.ds(512 * part, 512)])
            load("wb", wb_hbm, w_back)
            top_copies = []
            for a in range(SITES):
                for place, src in ((a, self_hbm), (3 + a, cross_hbm)):
                    top_copies.append(
                        pltpu.make_async_copy(src.at[a, 1], top_chi.at[place], in_sem.at[counter[0]])
                    )
                    counter[0] += 1

            @pl.when(leading)
            def _():
                for copy in top_copies:
                    copy.start()

        forward_site(q)
        if q == 0:
            pl.semaphore_wait(barrier, PEERS)
        send_forward(q, 1)
    for q in range(SITES):
        send_forward(q, 0)
        keep_own(q)

    copies["r"].wait()
    copies["u"].wait()

    def history(c, sums):
        rows = pl.ds(pl.multiple_of(c * 8, 8), 8)
        rs = [hr[i, rows, :] for i in range(HIST)]
        for i in range(HIST):
            ut[i, rows, :] = ut[i, rows, :] + MIXING * rs[i]
        return tuple(s + rs[i] * rs[j] for s, (i, j) in zip(sums, PAIRS))

    zero = jnp.zeros((8, 256), F32)
    past = lax.fori_loop(0, SITES * ROWS // 8, history, (zero,) * len(PAIRS))

    def pack(entries, first):
        row = jnp.zeros((1, 128), F32)
        for place, entry in enumerate(entries):
            folded = entry[:, 0:128] + entry[:, 128:256]
            value = jnp.sum(jnp.sum(folded, axis=0, keepdims=True), axis=1, keepdims=True)
            row = jnp.where(lane == first + place, value, row)
        return row

    past_row = pack(past, 0)

    for part in range(3):
        copies[("cs", part)].wait()
        copies[("hw", part)].wait()
        copies[("ht", part)].wait()
    copies["wb"].wait()
    for a in range(SITES):
        copies[("sl", a)].wait()
        copies[("cl", a)].wait()

    @pl.when(leading)
    def _():
        for copy in top_copies:
            copy.wait()

    def arrived(sem):
        block = sent.at[0, pl.ds(0, PEERS * 8)]
        pltpu.make_async_copy(block, block, sem).wait()

    def along_y(pick, target, q):
        for s in range(4):
            columns = pl.ds(128 * s, 128)
            one, two = zz_f[0:256, columns], zz_f[256:512, columns]
            high, low = halves(pick(one, two))
            u_b[:, pl.ds(128 * s, 128)] = high
            u_b[:, pl.ds(512 + 128 * s, 128)] = high
            u_b[:, pl.ds(1024 + 128 * s, 128)] = low
        target[q] = lax.dot_general(h_wide[...], u_b[...], NT, preferred_element_type=F32)

    def pick_whole(one, two):
        other = swap(two)
        return one + jnp.where(real_half, other, -other)

    def pick_low(one, two):
        return jnp.where(real_half, one, -swap(two))

    def pick_top(one, two):
        return jnp.where(real_half, swap(one), -two)

    def plane_site(q, carry):
        arrived(frecv.at[q])
        for s in range(4):
            columns = pl.ds(128 * s, 128)
            high, low = halves(got[q, s])
            r_b[0:256, columns] = high
            r_b[256:512, columns] = high
            r_b[512:768, columns] = low
        zz_f[...] = lax.dot_general(cs_wide[...], r_b[...], NN, preferred_element_type=F32)

        @pl.when(leading)
        def _():
            along_y(pick_low, spec, q)
            along_y(pick_top, spec_top, q)

        @pl.when(jnp.logical_not(leading))
        def _():
            along_y(pick_whole, spec, q)

        return carry

    lax.fori_loop(0, SITES, plane_site, 0)

    def combine(chi, field, a, rows, upper):
        total = None
        for g in range(SITES):
            entry = chi[jnp.where(a == g, a, a + g + 2), rows, :]
            term = entry * field[g, upper, :]
            total = term if total is None else total + term
        return total

    def store_mixed(rows, value):
        high, low = halves(value)
        m_b[rows, 0:256] = high
        m_b[rows, 256:512] = high
        m_b[rows, 512:768] = low

    shelf = pl.multiple_of((plane * 4 + site) * 8, 8)

    def back_site(a, carry):
        def mix(c, carry):
            rows = pl.ds(pl.multiple_of(c * 32, 32), 32)
            lower = pl.ds(pl.multiple_of(256 + c * 32, 32), 32)
            real = combine(low_chi, spec, a, rows, rows)
            imag = combine(low_chi, spec, a, rows, lower)

            @pl.when(leading)
            def _():
                top_real = combine(top_chi, spec_top, a, rows, rows)
                top_imag = combine(top_chi, spec_top, a, rows, lower)
                store_mixed(rows, (real - top_imag) * (1.0 / N**3))
                store_mixed(lower, (imag + top_real) * (1.0 / N**3))

            @pl.when(jnp.logical_not(leading))
            def _():
                store_mixed(rows, real * (2.0 / N**3))
                store_mixed(lower, imag * (2.0 / N**3))

            return carry

        lax.fori_loop(0, 8, mix, 0)
        zz_f[...] = lax.dot_general(cs_wide[...], m_b[...], NT, preferred_element_type=F32)
        for block in range(4):
            rows, lower = pl.ds(64 * block, 64), pl.ds(256 + 64 * block, 64)
            real = zz_f[rows, 0:256] - zz_f[lower, 256:512]
            imag = zz_f[rows, 256:512] + zz_f[lower, 0:256]
            for place, value in ((0, real), (256, imag)):
                high, low = halves(value)
                t_b[rows, pl.ds(place, 256)] = high
                t_b[rows, pl.ds(512 + place, 256)] = high
                t_b[rows, pl.ds(1024 + place, 256)] = low
        planes = lax.dot_general(t_b[...], h_tall[...], NN, preferred_element_type=F32)
        for s in range(4):
            back[a, s] = planes[:, 128 * s : 128 * s + 128]

        def action(sl, st):
            pltpu.make_async_remote_copy(
                src_ref=back.at[a, st, pl.ds(pl.multiple_of(sl * 8, 8), 8)],
                dst_ref=home.at[a, core, pl.ds(shelf, 8)],
                send_sem=bsend.at[a],
                recv_sem=brecv.at[core * 3 + a],
                device_id=(sl, st),
                device_id_type=MESH,
            ).start()

        over_peers(action, cores)
        home[a, core, pl.ds(shelf, 8), :] = back[
            a, site, pl.ds(pl.multiple_of(slab * 8, 8), 8), :
        ]
        return carry

    lax.fori_loop(0, SITES, back_site, 0)

    def arrived_home(a, side):
        @pl.when(core == side)
        def _():
            block = sent.at[0, pl.ds(0, 63 * 8)]
            pltpu.make_async_copy(block, block, brecv.at[side * 3 + a]).wait()

        @pl.when(core != side)
        def _():
            block = sent.at[0, pl.ds(0, 64 * 8)]
            pltpu.make_async_copy(block, block, brecv.at[side * 3 + a]).wait()

    def along_z(a, side):
        arrived_home(a, side)
        for pair in range(4):
            lines = jnp.transpose(
                jnp.concatenate(
                    [home[a, side, pl.ds(2 * pair + x, 64, stride=8), :] for x in range(2)], 0
                )
            )
            real, imag = lines[0:64], lines[64:128]
            first = jnp.where(real_half, real, swap(imag))
            second = jnp.where(real_half, swap(real), imag)
            for x, value in ((2 * pair, first), (2 * pair + 1, second)):
                high, low = halves(value)
                rows = pl.ds(64 * x, 64)
                e_b[rows, 0:128] = high
                e_b[rows, 128:256] = high
                e_b[rows, 256:384] = low
        y_f[...] = lax.dot_general(e_b[...], w_back[side], NN, preferred_element_type=F32)

    def home_first(a, carry):
        along_z(a, 1)

        def chunk(c, carry):
            rows = pl.ds(pl.multiple_of(c * 32, 32), 32)
            hv[a, rows, :] = y_f[rows, :] - hv[a, rows, :]
            return carry

        return lax.fori_loop(0, ROWS // 32, chunk, carry)

    lax.fori_loop(0, SITES, home_first, 0)

    def home_second(a, sums):
        along_z(a, 0)

        def chunk(c, sums):
            rows = pl.ds(pl.multiple_of(c * 8, 8), 8)
            latest = y_f[rows, :] + hv[a, rows, :]
            last_ref[a, rows, :] = latest
            tv[a, rows, :] = tv[a, rows, :] + MIXING * latest
            offset = pl.ds(pl.multiple_of(a * ROWS + c * 8, 8), 8)
            new = [s + hr[i, offset, :] * latest for i, s in enumerate(sums[:HIST])]
            return tuple(new) + (sums[HIST] + latest * latest,)

        return lax.fori_loop(0, ROWS // 8, chunk, sums, unroll=8)

    newest = lax.fori_loop(0, SITES, home_second, (zero,) * (HIST + 1))

    row = past_row + pack(newest, len(PAIRS))
    g_row[0:1, :] = row

    def send_row(sl, st):
        pltpu.make_async_remote_copy(
            src_ref=g_row.at[pl.ds(0, 1)],
            dst_ref=g_all.at[pl.ds(me, 1)],
            send_sem=gsend,
            recv_sem=grecv,
            device_id=(sl, st),
            device_id_type=MESH,
        ).start()

    over_peers(send_row, cores)
    g_all[pl.ds(me, 1), :] = row

    def wait_rows(sem):
        block = g_all.at[pl.ds(0, PEERS)]
        pltpu.make_async_copy(block, block, sem).wait()

    wait_rows(grecv)
    whole = jnp.sum(g_all[...], axis=0, keepdims=True)

    gram = [[None] * (HIST + 1) for i in range(HIST + 1)]
    for index, (i, j) in enumerate(PAIRS + [(i, HIST) for i in range(HIST + 1)]):
        value = jnp.sum(jnp.where(lane == index, whole, 0.0), axis=1, keepdims=True)
        gram[i][j] = gram[j][i] = jnp.broadcast_to(value, (1, 128))
    for i, weight in enumerate(solve_weights(gram)):
        weight_ref[i : i + 1, :] = weight

    for q in range(SITES):
        arrived(fsend.at[q])
        arrived(bsend.at[q])
    wait_rows(gsend)


def last_kernel(weight_ref, ut, tv, last_vmem, next_hbm, last_hbm, res, sem):
    pltpu.make_async_copy(last_vmem, last_hbm, sem.at[SITES]).start()
    weights = []
    for i in range(HIST + 1):
        weight = weight_ref[i : i + 1, :]
        weights.append(jnp.broadcast_to(jnp.concatenate([weight, weight], 1), (8, 256)))
    for a in range(SITES):

        def finish(c, carry):
            rows = pl.ds(pl.multiple_of(c * 8, 8), 8)
            offset = pl.ds(pl.multiple_of(a * ROWS + c * 8, 8), 8)
            value = weights[0] * ut[0, offset, :]
            for i in range(1, HIST):
                value = value + weights[i] * ut[i, offset, :]
            res[a, rows, :] = value + weights[HIST] * tv[a, rows, :]
            return carry

        lax.fori_loop(0, ROWS // 8, finish, 0, unroll=4)
        pltpu.make_async_copy(res.at[a], next_hbm.at[a], sem.at[a]).start()
    for a in range(SITES):
        pltpu.make_async_copy(res.at[a], next_hbm.at[a], sem.at[a]).wait()
    pltpu.make_async_copy(last_vmem, last_hbm, sem.at[SITES]).wait()


def step(potential, t_now, hist_t, hist_r, chi_self, chi_cross):
    flat = (SITES, ROWS, N)
    wz, cs, hh, wb = tables()
    vm = pltpu.VMEM
    field = pltpu.VMEM(flat, F32)
    whole = pl.BlockSpec(memory_space=pltpu.VMEM)
    scratch = [
        vm(flat, F32), vm((HIST, SITES * ROWS, N), F32),
        vm((6, N, N), F32), vm((6, N, N), F32),
        vm((256, 768), BF16), vm((2, 384, 256), BF16), vm((512, 768), BF16),
        vm((512, 1536), BF16), vm((1536, 512), BF16),
        vm((SITES, 1024, 128), F32), vm((SITES, 4, 256, 128), F32),
        vm((SITES, 512, 256), F32), vm((SITES, 512, 256), F32),
        vm((SITES, 4, 256, 128), F32), vm((SITES, 2, 512, 128), F32),
        vm((512, 768), BF16), vm((256, 512), F32), vm((768, 512), BF16),
        vm((512, 512), F32), vm((256, 1536), BF16), vm((512, 768), BF16),
        vm((256, 1536), BF16), vm((512, 384), BF16), vm((512, 256), F32),
        vm((8, 128), F32), vm((128, 128), F32),
        pltpu.SemaphoreType.DMA((40,)),
        pltpu.SemaphoreType.DMA((3,)), pltpu.SemaphoreType.DMA((3,)),
        pltpu.SemaphoreType.DMA((3,)), pltpu.SemaphoreType.DMA((6,)),
        pltpu.SemaphoreType.DMA, pltpu.SemaphoreType.DMA,
    ]
    anywhere = pl.BlockSpec(memory_space=pltpu.HBM)
    inner = pl.pallas_call(
        kernel,
        out_shape=(vm((8, 128), F32), vm((HIST, SITES * ROWS, N), F32), field, field),
        in_specs=[anywhere] * 10,
        out_specs=(whole,) * 4,
        scratch_shapes=scratch,
        compiler_params=pltpu.CompilerParams(
            collective_id=0, has_side_effects=True, vmem_limit_bytes=54 * 1024 * 1024
        ),
    )(
        potential.reshape(flat),
        t_now.reshape(flat),
        hist_t.reshape(HIST, SITES * ROWS, N),
        hist_r.reshape(HIST, SITES * ROWS, N),
        chi_self,
        chi_cross,
        jnp.asarray(wz),
        jnp.asarray(cs),
        jnp.asarray(hh),
        jnp.asarray(wb),
    )
    outer = jax.ShapeDtypeStruct(flat, F32)
    t_next, residual = pl.pallas_call(
        last_kernel,
        out_shape=(outer, outer),
        in_specs=[whole] * 4,
        out_specs=(anywhere, anywhere),
        scratch_shapes=[vm(flat, F32), pltpu.SemaphoreType.DMA((SITES + 1,))],
        compiler_params=pltpu.CompilerParams(vmem_limit_bytes=16 * 1024 * 1024),
    )(*inner)
    return t_next.reshape(t_now.shape), residual.reshape(t_now.shape)


def solution(mesh):
    field = P(None, "slab", "site", None)
    past = P(None, None, "slab", "site", None)
    chi = P(None, ("slab", "site"), None, None)
    return jax.shard_map(
        step,
        mesh=mesh,
        in_specs=(field, field, past, past, chi, chi),
        out_specs=(field, field),
        check_vma=False,
    )
```

```python
import functools
import math

import jax
import jax.numpy as jnp
import numpy as np
from jax import lax
from jax.experimental import pallas as pl
from jax.experimental.pallas import tpu as pltpu
from jax.sharding import PartitionSpec as P

N = 256
HALF = N // 2
SITES = 3
HIST = 4
MIXING = 0.5
MESH = pl.DeviceIdType.MESH
F32 = jnp.float32
BF16 = jnp.bfloat16

ROWS = 512
PEERS = 127

NT = (((1,), (1,)), ((), ()))
NN = (((1,), (0,)), ((), ()))


def split_table(table):
    high = table.astype(np.float32).astype(jnp.bfloat16)
    low = (table - high.astype(np.float64)).astype(np.float32).astype(jnp.bfloat16)
    return np.stack([high, low])


def tables():
    index = np.arange(N)
    angles = (index[:, None] * index[None, :] % N) * (2.0 * math.pi / N)
    cosine, sine = np.cos(angles), np.sin(angles)
    imag_rows = -sine[:HALF].copy()
    imag_rows[0] = 1.0 - 2.0 * (index % 2)
    along_z = np.concatenate([cosine[:HALF], imag_rows], 0)
    along_x = np.concatenate([cosine, sine], 0)
    blocks = np.stack([cosine.reshape(N, 4, 64), sine.reshape(N, 4, 64)], 2).reshape(N, 512)
    turned = np.stack([-sine.reshape(N, 4, 64), cosine.reshape(N, 4, 64)], 2).reshape(N, 512)
    along_y = np.concatenate([blocks, turned], 0)
    waves = np.arange(HALF).reshape(16, 2, 4)
    cuts = [split_table(along_z[np.concatenate([w, w + HALF])]) for w in (waves[:, c].ravel() for c in (0, 1))]
    from_z = np.stack([np.concatenate([cut[0], cut[1], cut[0]], 0) for cut in cuts])
    return split_table(along_z), split_table(along_x), split_table(along_y), from_z


def halves(value):
    high = value.astype(BF16)
    low = (value - high.astype(F32)).astype(BF16)
    return high, low


def solve_weights(gram):
    count = HIST + 1
    inverse = []
    factor = [[None] * count for member in range(count)]
    for column in range(count):
        diagonal_sum = gram[column][column]
        for inner in range(column):
            diagonal_sum = diagonal_sum - factor[column][inner] * factor[column][inner]
        factor[column][column] = jnp.sqrt(diagonal_sum)
        inverse.append(1.0 / factor[column][column])
        for row in range(column + 1, count):
            entry = gram[row][column]
            for inner in range(column):
                entry = entry - factor[row][inner] * factor[column][inner]
            factor[row][column] = entry * inverse[column]
    middle = []
    for row in range(count):
        entry = jnp.ones_like(gram[0][0])
        for inner in range(row):
            entry = entry - factor[row][inner] * middle[inner]
        middle.append(entry * inverse[row])
    weights = [None] * count
    for row in range(count - 1, -1, -1):
        entry = middle[row]
        for inner in range(row + 1, count):
            entry = entry - factor[inner][row] * weights[inner]
        weights[row] = entry * inverse[row]
    total = weights[0]
    for row in range(1, count):
        total = total + weights[row]
    return [weight / total for weight in weights]


PAIRS = [(i, j) for i in range(HIST) for j in range(i, HIST)]


def kernel(
    pot_hbm, t_hbm, hist_t_hbm, hist_r_hbm, self_hbm, cross_hbm, wz_hbm, cs_hbm, h_hbm, wb_hbm,
    weight_ref, ut, tv, last_ref,
    hv, hr, low_chi, top_chi,
    wz_wide, w_back, cs_wide, h_wide, h_tall,
    sent, got, spec, spec_top, back, home,
    d_b, z_f, r_b, zz_f, u_b, m_b, t_b, e_b, y_f,
    g_row, g_all,
    in_sem, fsend, frecv, bsend, brecv, gsend, grecv,
):
    slab = lax.axis_index("slab")
    site = lax.axis_index("site")
    plane = slab // 2
    py, px, core = plane // 4, plane % 4, slab % 2
    me = slab * 4 + site
    leading = me == 0

    counter = [0]
    copies = {}

    def load(name, src, dst):
        copy = pltpu.make_async_copy(src, dst, in_sem.at[counter[0]])
        counter[0] += 1
        copies[name] = copy
        copy.start()

    for q in range(SITES):
        load(("t", q), t_hbm.at[q], tv.at[q])
        load(("p", q), pot_hbm.at[q], hv.at[q])
        if q == 0:
            load("wz0", wz_hbm.at[0], wz_wide.at[:, pl.ds(0, 256)])
            load("wz1", wz_hbm.at[1], wz_wide.at[:, pl.ds(256, 256)])
            load("wz2", wz_hbm.at[0], wz_wide.at[:, pl.ds(512, 256)])
    cores = [core, (core + 1) % 2]
    zs = [(site + step) % 4 for step in (2, 1, 3, 0)]

    def distance(place):
        return jnp.where(place < 2, 2 - place, (place + 1) % 4)

    def over_peers(action, sides):
        def step(group, carry):
            chip = ((py + distance(group // 4)) % 4) * 4 + (px + distance(group % 4)) % 4
            for side in sides:
                for z in zs:
                    action(chip * 2 + side, z)
            return carry

        lax.fori_loop(0, 15, step, 0)
        for side in sides:
            for z in zs[:3]:
                action(plane * 2 + side, z)
            if side is cores[1]:
                action(plane * 2 + side, site)
            elif side is not cores[0]:

                @pl.when(core != side)
                def _():
                    action(plane * 2 + side, site)

    barrier = pltpu.get_barrier_semaphore()
    over_peers(
        lambda sl, st: pl.semaphore_signal(
            barrier, inc=1, device_id=(sl, st), device_id_type=MESH
        ),
        cores,
    )

    lane = lax.broadcasted_iota(jnp.int32, (1, 128), 1)
    real_half = lane < 64

    def swap(value):
        return pltpu.roll(value, 64, 1)

    def forward_site(q):
        def chunk(c, carry):
            rows = pl.ds(pl.multiple_of(c * 64, 64), 64)
            indirect = tv[q, rows, :]
            field = indirect - hv[q, rows, :]
            total = jnp.where(field > 0, field, jnp.exp(jnp.minimum(field, 0.0)) - 1.0)
            hv[q, rows, :] = total
            high, low = halves(total - indirect)
            d_b[rows, 0:256] = high
            d_b[rows, 256:512] = high
            d_b[rows, 512:768] = low
            return carry

        lax.fori_loop(0, ROWS // 64, chunk, 0)
        z_f[...] = lax.dot_general(wz_wide[...], d_b[...], NT, preferred_element_type=F32)
        for pair in range(4):
            columns = pl.ds(128 * pair, 128)
            real, imag = z_f[0:128, columns], z_f[128:256, columns]
            first = jnp.where(real_half, real, swap(imag))
            second = jnp.where(real_half, swap(real), imag)
            sent[q, pl.ds(2 * pair, 128, stride=8), :] = first
            sent[q, pl.ds(2 * pair + 1, 128, stride=8), :] = second

    def send_forward(q, side):
        def action(sl, st):
            wave = pl.multiple_of((sl * 4 + st) * 8, 8)
            pltpu.make_async_remote_copy(
                src_ref=sent.at[q, pl.ds(wave, 8)],
                dst_ref=got.at[q, site, pl.ds(pl.multiple_of(slab * 8, 8), 8)],
                send_sem=fsend.at[q],
                recv_sem=frecv.at[q],
                device_id=(sl, st),
                device_id_type=MESH,
            ).start()

        over_peers(action, (side,))

    def keep_own(q):
        got[q, site, pl.ds(pl.multiple_of(slab * 8, 8), 8), :] = sent[
            q, pl.ds(pl.multiple_of(me * 8, 8), 8), :
        ]

    for q in range(SITES):
        copies[("t", q)].wait()
        copies[("p", q)].wait()
        if q == 0:
            for part in range(3):
                copies[f"wz{part}"].wait()
            load("r", hist_r_hbm, hr)
            load("u", hist_t_hbm, ut)
            for part in range(3):
                load(("cs", part), cs_hbm.at[part % 2], cs_wide.at[:, pl.ds(256 * part, 256)])
                load(("hw", part), h_hbm.at[part % 2], h_wide.at[:, pl.ds(512 * part, 512)])
            for a in range(SITES):
                load(("sl", a), self_hbm.at[a, 0], low_chi.at[a])
                load(("cl", a), cross_hbm.at[a, 0], low_chi.at[3 + a])
            for part in range(3):
                load(("ht", part), h_hbm.at[part % 2], h_tall.at[pl.ds(512 * part, 512)])
            load("wb", wb_hbm, w_back)
            top_copies = []
            for a in range(SITES):
                for place, src in ((a, self_hbm), (3 + a, cross_hbm)):
                    top_copies.append(
                        pltpu.make_async_copy(src.at[a, 1], top_chi.at[place], in_sem.at[counter[0]])
                    )
                    counter[0] += 1

            @pl.when(leading)
            def _():
                for copy in top_copies:
                    copy.start()

        forward_site(q)
        if q == 0:
            pl.semaphore_wait(barrier, PEERS)
        send_forward(q, 1)
    for q in range(SITES):
        send_forward(q, 0)
        keep_own(q)

    copies["r"].wait()
    copies["u"].wait()

    def history(c, sums):
        rows = pl.ds(pl.multiple_of(c * 8, 8), 8)
        rs = [hr[i, rows, :] for i in range(HIST)]
        for i in range(HIST):
            ut[i, rows, :] = ut[i, rows, :] + MIXING * rs[i]
        return tuple(s + rs[i] * rs[j] for s, (i, j) in zip(sums, PAIRS))

    zero = jnp.zeros((8, 256), F32)
    past = lax.fori_loop(0, SITES * ROWS // 8, history, (zero,) * len(PAIRS))

    def pack(entries, first):
        row = jnp.zeros((1, 128), F32)
        for place, entry in enumerate(entries):
            folded = entry[:, 0:128] + entry[:, 128:256]
            value = jnp.sum(jnp.sum(folded, axis=0, keepdims=True), axis=1, keepdims=True)
            row = jnp.where(lane == first + place, value, row)
        return row

    past_row = pack(past, 0)

    for part in range(3):
        copies[("cs", part)].wait()
        copies[("hw", part)].wait()
        copies[("ht", part)].wait()
    copies["wb"].wait()
    for a in range(SITES):
        copies[("sl", a)].wait()
        copies[("cl", a)].wait()

    @pl.when(leading)
    def _():
        for copy in top_copies:
            copy.wait()

    def arrived(sem):
        block = sent.at[0, pl.ds(0, PEERS * 8)]
        pltpu.make_async_copy(block, block, sem).wait()

    def along_y(pick, target, q):
        for s in range(4):
            columns = pl.ds(128 * s, 128)
            one, two = zz_f[0:256, columns], zz_f[256:512, columns]
            high, low = halves(pick(one, two))
            u_b[:, pl.ds(128 * s, 128)] = high
            u_b[:, pl.ds(512 + 128 * s, 128)] = high
            u_b[:, pl.ds(1024 + 128 * s, 128)] = low
        target[q] = lax.dot_general(h_wide[...], u_b[...], NT, preferred_element_type=F32)

    def pick_whole(one, two):
        other = swap(two)
        return one + jnp.where(real_half, other, -other)

    def pick_low(one, two):
        return jnp.where(real_half, one, -swap(two))

    def pick_top(one, two):
        return jnp.where(real_half, swap(one), -two)

    def plane_site(q, carry):
        arrived(frecv.at[q])
        for s in range(4):
            columns = pl.ds(128 * s, 128)
            high, low = halves(got[q, s])
            r_b[0:256, columns] = high
            r_b[256:512, columns] = high
            r_b[512:768, columns] = low
        zz_f[...] = lax.dot_general(cs_wide[...], r_b[...], NN, preferred_element_type=F32)

        @pl.when(leading)
        def _():
            along_y(pick_low, spec, q)
            along_y(pick_top, spec_top, q)

        @pl.when(jnp.logical_not(leading))
        def _():
            along_y(pick_whole, spec, q)

        return carry

    lax.fori_loop(0, SITES, plane_site, 0)

    def combine(chi, field, a, rows, upper):
        total = None
        for g in range(SITES):
            entry = chi[jnp.where(a == g, a, a + g + 2), rows, :]
            term = entry * field[g, upper, :]
            total = term if total is None else total + term
        return total

    def store_mixed(rows, value):
        high, low = halves(value)
        m_b[rows, 0:256] = high
        m_b[rows, 256:512] = high
        m_b[rows, 512:768] = low

    shelf = pl.multiple_of((plane * 4 + site) * 8, 8)

    def back_site(a, carry):
        def mix(c, carry):
            rows = pl.ds(pl.multiple_of(c * 32, 32), 32)
            lower = pl.ds(pl.multiple_of(256 + c * 32, 32), 32)
            real = combine(low_chi, spec, a, rows, rows)
            imag = combine(low_chi, spec, a, rows, lower)

            @pl.when(leading)
            def _():
                top_real = combine(top_chi, spec_top, a, rows, rows)
                top_imag = combine(top_chi, spec_top, a, rows, lower)
                store_mixed(rows, (real - top_imag) * (1.0 / N**3))
                store_mixed(lower, (imag + top_real) * (1.0 / N**3))

            @pl.when(jnp.logical_not(leading))
            def _():
                store_mixed(rows, real * (2.0 / N**3))
                store_mixed(lower, imag * (2.0 / N**3))

            return carry

        lax.fori_loop(0, 8, mix, 0)
        zz_f[...] = lax.dot_general(cs_wide[...], m_b[...], NT, preferred_element_type=F32)
        for block in range(4):
            rows, lower = pl.ds(64 * block, 64), pl.ds(256 + 64 * block, 64)
            real = zz_f[rows, 0:256] - zz_f[lower, 256:512]
            imag = zz_f[rows, 256:512] + zz_f[lower, 0:256]
            for place, value in ((0, real), (256, imag)):
                high, low = halves(value)
                t_b[rows, pl.ds(place, 256)] = high
                t_b[rows, pl.ds(512 + place, 256)] = high
                t_b[rows, pl.ds(1024 + place, 256)] = low
        planes = lax.dot_general(t_b[...], h_tall[...], NN, preferred_element_type=F32)
        for s in range(4):
            back[a, s] = planes[:, 128 * s : 128 * s + 128]

        def action(sl, st):
            pltpu.make_async_remote_copy(
                src_ref=back.at[a, st, pl.ds(pl.multiple_of(sl * 8, 8), 8)],
                dst_ref=home.at[a, core, pl.ds(shelf, 8)],
                send_sem=bsend.at[a],
                recv_sem=brecv.at[core * 3 + a],
                device_id=(sl, st),
                device_id_type=MESH,
            ).start()

        over_peers(action, cores)
        home[a, core, pl.ds(shelf, 8), :] = back[
            a, site, pl.ds(pl.multiple_of(slab * 8, 8), 8), :
        ]
        return carry

    lax.fori_loop(0, SITES, back_site, 0)

    def arrived_home(a, side):
        @pl.when(core == side)
        def _():
            block = sent.at[0, pl.ds(0, 63 * 8)]
            pltpu.make_async_copy(block, block, brecv.at[side * 3 + a]).wait()

        @pl.when(core != side)
        def _():
            block = sent.at[0, pl.ds(0, 64 * 8)]
            pltpu.make_async_copy(block, block, brecv.at[side * 3 + a]).wait()

    def along_z(a, side):
        arrived_home(a, side)
        for pair in range(4):
            lines = jnp.transpose(
                jnp.concatenate(
                    [home[a, side, pl.ds(2 * pair + x, 64, stride=8), :] for x in range(2)], 0
                )
            )
            real, imag = lines[0:64], lines[64:128]
            first = jnp.where(real_half, real, swap(imag))
            second = jnp.where(real_half, swap(real), imag)
            for x, value in ((2 * pair, first), (2 * pair + 1, second)):
                high, low = halves(value)
                rows = pl.ds(64 * x, 64)
                e_b[rows, 0:128] = high
                e_b[rows, 128:256] = high
                e_b[rows, 256:384] = low
            if pair % 2:
                part = pl.ds(128 * (pair - 1), 256)
                y_f[part, :] = lax.dot_general(
                    e_b[part, :], w_back[side], NN, preferred_element_type=F32
                )

    def home_first(a, carry):
        along_z(a, 1)

        def chunk(c, carry):
            rows = pl.ds(pl.multiple_of(c * 32, 32), 32)
            hv[a, rows, :] = y_f[rows, :] - hv[a, rows, :]
            return carry

        return lax.fori_loop(0, ROWS // 32, chunk, carry)

    lax.fori_loop(0, SITES, home_first, 0)

    def home_second(a, sums):
        along_z(a, 0)

        def chunk(c, sums):
            rows = pl.ds(pl.multiple_of(c * 8, 8), 8)
            latest = y_f[rows, :] + hv[a, rows, :]
            last_ref[a, rows, :] = latest
            tv[a, rows, :] = tv[a, rows, :] + MIXING * latest
            offset = pl.ds(pl.multiple_of(a * ROWS + c * 8, 8), 8)
            new = [s + hr[i, offset, :] * latest for i, s in enumerate(sums[:HIST])]
            return tuple(new) + (sums[HIST] + latest * latest,)

        return lax.fori_loop(0, ROWS // 8, chunk, sums, unroll=8)

    newest = lax.fori_loop(0, SITES, home_second, (zero,) * (HIST + 1))

    row = past_row + pack(newest, len(PAIRS))
    g_row[0:1, :] = row

    def send_row(sl, st):
        pltpu.make_async_remote_copy(
            src_ref=g_row.at[pl.ds(0, 1)],
            dst_ref=g_all.at[pl.ds(me, 1)],
            send_sem=gsend,
            recv_sem=grecv,
            device_id=(sl, st),
            device_id_type=MESH,
        ).start()

    over_peers(send_row, cores)
    g_all[pl.ds(me, 1), :] = row

    def wait_rows(sem):
        block = g_all.at[pl.ds(0, PEERS)]
        pltpu.make_async_copy(block, block, sem).wait()

    wait_rows(grecv)
    whole = jnp.sum(g_all[...], axis=0, keepdims=True)

    gram = [[None] * (HIST + 1) for i in range(HIST + 1)]
    for index, (i, j) in enumerate(PAIRS + [(i, HIST) for i in range(HIST + 1)]):
        value = jnp.sum(jnp.where(lane == index, whole, 0.0), axis=1, keepdims=True)
        gram[i][j] = gram[j][i] = jnp.broadcast_to(value, (1, 128))
    for i, weight in enumerate(solve_weights(gram)):
        weight_ref[i : i + 1, :] = weight

    for q in range(SITES):
        arrived(fsend.at[q])
        arrived(bsend.at[q])
    wait_rows(gsend)


def last_kernel(weight_ref, ut, tv, last_vmem, next_hbm, last_hbm, res, sem):
    pltpu.make_async_copy(last_vmem, last_hbm, sem.at[SITES]).start()
    weights = []
    for i in range(HIST + 1):
        weight = weight_ref[i : i + 1, :]
        weights.append(jnp.broadcast_to(jnp.concatenate([weight, weight], 1), (8, 256)))
    for a in range(SITES):

        def finish(c, carry):
            rows = pl.ds(pl.multiple_of(c * 8, 8), 8)
            offset = pl.ds(pl.multiple_of(a * ROWS + c * 8, 8), 8)
            value = weights[0] * ut[0, offset, :]
            for i in range(1, HIST):
                value = value + weights[i] * ut[i, offset, :]
            res[a, rows, :] = value + weights[HIST] * tv[a, rows, :]
            return carry

        lax.fori_loop(0, ROWS // 8, finish, 0, unroll=8)
        pltpu.make_async_copy(res.at[a], next_hbm.at[a], sem.at[a]).start()
    for a in range(SITES):
        pltpu.make_async_copy(res.at[a], next_hbm.at[a], sem.at[a]).wait()
    pltpu.make_async_copy(last_vmem, last_hbm, sem.at[SITES]).wait()


def step(potential, t_now, hist_t, hist_r, chi_self, chi_cross):
    flat = (SITES, ROWS, N)
    wz, cs, hh, wb = tables()
    vm = pltpu.VMEM
    field = pltpu.VMEM(flat, F32)
    whole = pl.BlockSpec(memory_space=pltpu.VMEM)
    scratch = [
        vm(flat, F32), vm((HIST, SITES * ROWS, N), F32),
        vm((6, N, N), F32), vm((6, N, N), F32),
        vm((256, 768), BF16), vm((2, 384, 256), BF16), vm((512, 768), BF16),
        vm((512, 1536), BF16), vm((1536, 512), BF16),
        vm((SITES, 1024, 128), F32), vm((SITES, 4, 256, 128), F32),
        vm((SITES, 512, 256), F32), vm((SITES, 512, 256), F32),
        vm((SITES, 4, 256, 128), F32), vm((SITES, 2, 512, 128), F32),
        vm((512, 768), BF16), vm((256, 512), F32), vm((768, 512), BF16),
        vm((512, 512), F32), vm((256, 1536), BF16), vm((512, 768), BF16),
        vm((256, 1536), BF16), vm((512, 384), BF16), vm((512, 256), F32),
        vm((8, 128), F32), vm((128, 128), F32),
        pltpu.SemaphoreType.DMA((40,)),
        pltpu.SemaphoreType.DMA((3,)), pltpu.SemaphoreType.DMA((3,)),
        pltpu.SemaphoreType.DMA((3,)), pltpu.SemaphoreType.DMA((6,)),
        pltpu.SemaphoreType.DMA, pltpu.SemaphoreType.DMA,
    ]
    anywhere = pl.BlockSpec(memory_space=pltpu.HBM)
    inner = pl.pallas_call(
        kernel,
        out_shape=(vm((8, 128), F32), vm((HIST, SITES * ROWS, N), F32), field, field),
        in_specs=[anywhere] * 10,
        out_specs=(whole,) * 4,
        scratch_shapes=scratch,
        compiler_params=pltpu.CompilerParams(
            collective_id=0, has_side_effects=True, vmem_limit_bytes=54 * 1024 * 1024
        ),
    )(
        potential.reshape(flat),
        t_now.reshape(flat),
        hist_t.reshape(HIST, SITES * ROWS, N),
        hist_r.reshape(HIST, SITES * ROWS, N),
        chi_self,
        chi_cross,
        jnp.asarray(wz),
        jnp.asarray(cs),
        jnp.asarray(hh),
        jnp.asarray(wb),
    )
    outer = jax.ShapeDtypeStruct(flat, F32)
    t_next, residual = pl.pallas_call(
        last_kernel,
        out_shape=(outer, outer),
        in_specs=[whole] * 4,
        out_specs=(anywhere, anywhere),
        scratch_shapes=[vm(flat, F32), pltpu.SemaphoreType.DMA((SITES + 1,))],
        compiler_params=pltpu.CompilerParams(vmem_limit_bytes=16 * 1024 * 1024),
    )(*inner)
    return t_next.reshape(t_now.shape), residual.reshape(t_now.shape)


def solution(mesh):
    field = P(None, "slab", "site", None)
    past = P(None, None, "slab", "site", None)
    chi = P(None, ("slab", "site"), None, None)
    return jax.shard_map(
        step,
        mesh=mesh,
        in_specs=(field, field, past, past, chi, chi),
        out_specs=(field, field),
        check_vma=False,
    )
```
